32 devices in a mesh: dp: 16 (over z, y, x), expert: 2 (over core).
Axes of the slice: x: 2, y: 2, z: 4, core: 2. Of those that a mesh axis runs over, the one named last changes fastest.
Arguments:
- master: float32 [2, 7168, 2048], P('expert', 'dp'), may hold values from -6 to 6
- first_moment: float32 [2, 7168, 2048], P('expert', 'dp'), may hold values from -0.06 to 0.06
- second_moment: float32 [2, 7168, 2048], P('expert', 'dp'), may hold values from 1e-05 to 0.001
- rotation: int32 [4, 16, 1], replicated, may hold values from 0 to 15; in each aligned block of 16 rows (0 to 15, 16 to 31, ..., all dimensions but the last counted through in order) at most 3 rows name the same one
- assignment: int32 [64], replicated, may hold values from 0 to 63, each once
Outputs:
- saved_master: float32 [2, 64, 3, 1792, 128], P('expert', 'dp')
- saved_update: float32 [2, 64, 3, 1792, 128], P('expert', 'dp')
- checksums: float32 [2, 2, 64], replicated
The draws below stay inside these ranges and needn't reach their ends.
Inputs may be any that keep to these rules, and one draw needn't show every extreme that they name: rotation[r, j, 0] is the dp index that writes span j of round r; within one round no index is named more than 3 times, and in some round one index is named exactly 3 times. `assignment`: a permutation of the spans' checksum slots.
All inputs are finite; a program needn't handle non-finite values.
Results may differ from the reference program's by a relative error of at most 0.00002.
Values sent between devices are 32-bit elements; how exact they have to be, the bound alone decides.
A program may use at most 128 MiB of HBM per device.

```python
import math
import jax
import jax.numpy as jnp
import numpy as np
from jax import lax

ROWS = 7168
COLS = 2048
LANE = 128
ROUNDS = 4
MOST = 3
STEP = 20
GROUPS = 2
SPANS = 64
N_DP = 16


def block_levels(stream_key, shape, pieces, smallest, top_value):
    gain, own = 1.0, jax.random.fold_in(stream_key, 6)
    for position, blocks in pieces:
        draws = jnp.exp(jax.random.uniform(jax.random.fold_in(own, position), (blocks,), jnp.float32, smallest / len(pieces), top_value / len(pieces)))
        gain = gain * jnp.repeat(draws, shape[position] // blocks).reshape([-1 if axis == position else 1 for axis in range(len(shape))])
    return gain


def shared_out(key, own, number, rows, count, top, bound, slope):
    ranking = jax.random.permutation(key, count)
    packed, usual = shares(count, rows * top, bound, slope, True), shares(count, rows * top, bound, slope, False)
    places = jnp.arange(count)

    def named(tallies, turn):
        used = int((tallies > 0).sum())
        fixed = max(1, used // 4)
        shifted = fixed + (places - fixed + turn * (used - fixed)) % max(1, count - fixed)
        return jnp.zeros((count,), jnp.int32).at[ranking[jnp.where(places < fixed, places, shifted)]].set(jnp.asarray(tallies, jnp.int32))

    tallies = jnp.where(number % 4 == 0, named(packed, number // 4), named(usual, number - number // 4 - 1))
    mixed = jax.random.permutation(jax.random.fold_in(own, 3), count)
    donor, sink = mixed[0:count // 2 * 2:2], mixed[1:count // 2 * 2:2]
    slack = jnp.minimum(tallies[donor] - 1, bound - tallies[sink]) // 2
    slack = jnp.where((donor == ranking[0]) | (sink == ranking[0]) | (tallies[sink] == 0), 0, jnp.maximum(slack, 0))
    shifted = jax.random.randint(jax.random.fold_in(own, 4), (count // 2,), 0, 1 << 20) % (slack + 1)
    tallies = tallies.at[donor].add(-shifted).at[sink].add(shifted)
    items = jnp.searchsorted(jnp.cumsum(tallies), jnp.arange(rows * top), side="right").astype(jnp.int32)
    listing = items.reshape(top, rows).T
    listing = listing[jax.random.permutation(jax.random.fold_in(own, 1), rows)]
    turn = jax.random.randint(jax.random.fold_in(own, 2), (rows, 1), 0, top)
    return jnp.take_along_axis(listing, (jnp.arange(top)[None, :] + turn) % top, axis=1)


def shares(amount, total, reach, slope, full):
    weights = [(1 << 20) // math.isqrt(standing ** slope) + 1 for standing in range(1, amount + 1)]
    largest = reach if full else min(reach, max(-(-total // amount), total * weights[0] // sum(weights)))
    least = 1 if total - largest >= amount - 1 else 0
    holding, rest = [largest] + [least] * (amount - 1), total - largest - least * (amount - 1)
    while rest > 0:
        movable = [i for i in range(1, amount) if holding[i] < largest] or [i for i in range(1, amount) if holding[i] < reach]
        whole, remaining = sum([weights[i] for i in movable]), rest
        for i in movable:
            extra = min(reach - holding[i], max(1, remaining * weights[i] // whole), rest)
            holding[i] = holding[i] + extra
            rest = rest - extra
    return np.array(holding)


def normal_values(rng, extent, deviation, reach, pieces=(), held_as=jnp.bfloat16):
    factor_of = block_levels(rng, extent, pieces, -0.22, 0.18) if pieces else 1.0
    drawn = jax.random.normal(rng, extent, jnp.float32) * deviation * factor_of
    return jnp.minimum(jnp.maximum(drawn, -reach), reach).astype(held_as)


def setup_inputs(seed: int = 0) -> dict:
    streams_of = jax.random.split(jax.random.key(seed), 6)
    master = normal_values(streams_of[0], (GROUPS, ROWS, COLS), 1.0, 6.0, ((0, 2), (1, 16)), jnp.float32)
    first_moment = normal_values(streams_of[1], (GROUPS, ROWS, COLS), 0.01, 0.06, ((0, 2), (1, 16)), jnp.float32)
    second_moment = jnp.clip(jnp.exp(math.log(0.001) - 4.6051703 * jax.random.uniform(streams_of[2], (GROUPS, ROWS, COLS), jnp.float32) ** block_levels(streams_of[2], (GROUPS, ROWS, COLS), ((0, 2), (1, 16)), -0.2, 0.2)), 9.999999747378752e-06, 0.001)
    rotation_keys = jax.random.split(jax.random.fold_in(streams_of[3], 1), ROUNDS * N_DP // N_DP)
    rotation_turns = jax.random.permutation(jax.random.fold_in(streams_of[3], 3), ROUNDS * N_DP // N_DP)
    rotation = jax.vmap(lambda own, number: shared_out(jax.random.fold_in(streams_of[3], 2), own, number, N_DP, N_DP, 1, MOST, 2))(rotation_keys, rotation_turns).reshape((ROUNDS, N_DP, 1))
    assignment = jax.random.permutation(streams_of[4], SPANS).astype(jnp.int32)
    return {"master": master, "first_moment": first_moment, "second_moment": second_moment, "rotation": rotation, "assignment": assignment}


BETA_ONE = 0.9
BETA_TWO = 0.95
EPSILON = 1e-08

def scaled_moment(first_part, second_part):
    corr_one = 1.0 - BETA_ONE ** STEP
    corr_two = 1.0 - BETA_TWO ** STEP
    return first_part / corr_one / (jnp.sqrt(second_part / corr_two) + EPSILON)

def slot_table(rotation, dp_count, most_slots):
    owners = rotation[:, :, 0]
    span_ids = jnp.arange(dp_count, dtype=jnp.int32)
    same_writer = owners[:, :, None] == owners[:, None, :]
    before = span_ids[None, :] < span_ids[:, None]
    slot_rank = lax.optimization_barrier(jnp.sum((same_writer & before[None]).astype(jnp.int32), axis=2))
    writers = jnp.arange(dp_count, dtype=jnp.int32)
    slot_ids = jnp.arange(most_slots, dtype=jnp.int32)
    matches = (owners[:, None, None, :] == writers[None, None, :, None]) & (slot_rank[:, None, None, :] == slot_ids[None, :, None, None])
    matches = matches.astype(jnp.int32)
    found_any = lax.optimization_barrier(jnp.sum(matches, axis=3))
    picked = lax.optimization_barrier(jnp.sum(matches * span_ids, axis=3))
    return (picked + (1 - found_any) * dp_count).astype(jnp.int32)

def position_weights(line_ids, per_row, lane_count):
    row_ids = line_ids // per_row
    col_ids = line_ids % per_row * lane_count
    lane_ids = jnp.arange(lane_count, dtype=jnp.int32)
    pattern = (row_ids[..., None] * 5 + (col_ids[..., None] + lane_ids) * 3) % 11
    return 1.0 + pattern.astype(jnp.float32) / 10.0

def reference(master, first_moment, second_moment, rotation, assignment):
    per_row = COLS // LANE
    lines_device = ROWS // N_DP * per_row
    piece_len = lines_device // (ROUNDS * N_DP)
    inv_count = 1.0 / math.sqrt(N_DP * piece_len * LANE)
    table = slot_table(rotation, N_DP, MOST)
    line_ids = jnp.arange(ROWS * per_row, dtype=jnp.int32).reshape(N_DP, ROUNDS, N_DP, piece_len)
    weights = position_weights(line_ids, per_row, LANE)
    round_ids = jnp.arange(ROUNDS, dtype=jnp.int32)[:, None, None]

    def arrange_field(field_in):
        line_view = field_in.reshape(N_DP, ROUNDS, N_DP, piece_len, LANE)
        totals = lax.optimization_barrier(jnp.sum(line_view * weights, axis=(0, 3, 4))) * inv_count
        reordered = jnp.transpose(line_view, (1, 2, 0, 3, 4))
        padded = jnp.concatenate([reordered, jnp.zeros((ROUNDS, 1, N_DP, piece_len, LANE), reordered.dtype)], axis=1)
        selected = padded[round_ids, table]
        saved_rows = jnp.transpose(selected, (2, 0, 1, 3, 4, 5)).reshape(N_DP * ROUNDS, MOST, N_DP * piece_len, LANE)
        return (saved_rows, totals.reshape(ROUNDS * N_DP))

    def one_group(fields):
        master_part, first_part, second_part = fields
        update = scaled_moment(first_part, second_part)
        saved_master, master_sums = arrange_field(master_part)
        saved_update, update_sums = arrange_field(update)
        return (saved_master, saved_update, jnp.stack([master_sums, update_sums]))
    saved_master, saved_update, group_sums = lax.map(one_group, (master, first_moment, second_moment))
    checksums = jnp.zeros_like(group_sums).at[:, :, assignment.astype(jnp.int32)].set(group_sums)
    return (saved_master, saved_update, checksums)
```

```python
import functools
import math

import jax
import jax.numpy as jnp
import numpy as np
from jax import lax
from jax.experimental import pallas as pl
from jax.experimental.pallas import tpu as pltpu
from jax.sharding import PartitionSpec as P

LANE = 128
MOST = 3
STEP = 20
INNER = 4


BETA_ONE = 0.9
BETA_TWO = 0.95
EPSILON = 1e-08


def scaled_moment(first_part, second_part):
    corr_one = 1.0 - BETA_ONE**STEP
    corr_two = 1.0 - BETA_TWO**STEP
    return first_part / corr_one / (jnp.sqrt(second_part / corr_two) + EPSILON)


def slot_table(rotation, dp_count, most_slots):
    owners = rotation[:, :, 0]
    span_ids = jnp.arange(dp_count, dtype=jnp.int32)
    same_writer = owners[:, :, None] == owners[:, None, :]
    before = span_ids[None, :] < span_ids[:, None]
    slot_rank = jnp.sum((same_writer & before[None]).astype(jnp.int32), axis=2)
    writers = jnp.arange(dp_count, dtype=jnp.int32)
    slot_ids = jnp.arange(most_slots, dtype=jnp.int32)
    matches = (owners[:, None, None, :] == writers[None, None, :, None]) & (
        slot_rank[:, None, None, :] == slot_ids[None, :, None, None]
    )
    matches = matches.astype(jnp.int32)
    found_any = jnp.sum(matches, axis=3)
    picked = jnp.sum(matches * span_ids, axis=3)
    return picked + (1 - found_any) * dp_count


def position_weights(line_ids, per_row, lane_count):
    row_ids = line_ids // per_row
    col_ids = line_ids % per_row * lane_count
    lane_ids = jnp.arange(lane_count, dtype=jnp.int32)
    pattern = (row_ids[..., None] * 5 + (col_ids[..., None] + lane_ids) * 3) % 11
    return 1.0 + pattern.astype(jnp.float32) / 10.0


def exchange_kernel(
    planes, inner, groups, slots, cap, pos_ref, sum_ref, m_ref, u_ref, om_ref, ou_ref, oc_ref, *scratch
):
    held = scratch[: 2 * planes]
    stage = scratch[2 * planes : 4 * planes]
    zs_sem, zr_sem, local_sem, is_sem, ir_sem, self_sem = scratch[4 * planes : 4 * planes + 6]
    by_plane, by_spot, by_group, cs_sem, cr_sem, cl_sem = scratch[4 * planes + 6 :]
    me = lax.axis_index("dp")
    plane = me // inner
    spot = me % inner
    core = lax.axis_index("expert")
    fields = (m_ref, u_ref)
    outs = (om_ref, ou_ref)

    def peer(plane_to, spot_to):
        return (plane_to * inner + spot_to, core)

    def mate(d):
        other, bit = plane, 1
        while bit < planes:
            if d & bit:
                other = other + bit * (1 - 2 * ((plane // bit) % 2))
            bit *= 2
        return other

    barrier = pltpu.get_barrier_semaphore()
    for d in range(1, planes):
        pl.semaphore_signal(
            barrier, inc=1, device_id=peer(mate(d), spot), device_id_type=pl.DeviceIdType.MESH
        )
    for e in range(1, inner):
        pl.semaphore_signal(
            barrier, inc=1, device_id=peer(plane, (spot + e) % inner), device_id_type=pl.DeviceIdType.MESH
        )
    for g in range(1, groups):
        pl.semaphore_signal(
            barrier, inc=1, device_id=(me, (core + g) % groups), device_id_type=pl.DeviceIdType.MESH
        )
    pl.semaphore_wait(barrier, planes + inner + groups - 3)

    def small(src, dst, number, to):
        copy = pltpu.make_async_remote_copy(
            src_ref=src,
            dst_ref=dst,
            send_sem=cs_sem.at[number],
            recv_sem=cr_sem.at[number],
            device_id=to,
            device_id_type=pl.DeviceIdType.MESH,
        )
        copy.start()
        return copy

    own_sums = pltpu.make_async_copy(sum_ref, by_plane.at[0], cl_sem.at[0])
    own_sums.start()
    sums_far = [
        small(sum_ref, by_plane.at[d], d, peer(mate(d), spot)) for d in range(1, planes)
    ]

    far = [None] * (2 * planes)
    for f in range(2):
        own = pltpu.make_async_copy(fields[f].at[plane], held[f * planes], local_sem.at[f])
        own.start()
        far[f * planes] = own
        for d in range(1, planes):
            to_plane = mate(d)
            copy = pltpu.make_async_remote_copy(
                src_ref=fields[f].at[to_plane],
                dst_ref=held[f * planes + d],
                send_sem=zs_sem.at[f * planes + d],
                recv_sem=zr_sem.at[f * planes + d],
                device_id=peer(to_plane, spot),
                device_id_type=pl.DeviceIdType.MESH,
            )
            copy.start()
            far[f * planes + d] = copy

    own_sums.wait()
    for copy in sums_far:
        copy.wait()
    kept_sums = pltpu.make_async_copy(by_plane, by_spot.at[0], cl_sem.at[1])
    kept_sums.start()
    sums_near = [
        small(by_plane, by_spot.at[e], planes + e, peer(plane, (spot + e) % inner)) for e in range(1, inner)
    ]

    near = []
    order = [(f, 0) for f in range(2)] + [(f, d) for f in range(2) for d in range(1, planes)]
    for f, d in order:
        g = f * planes + d
        if d == 0:
            far[g].wait()
        else:
            far[g].wait_recv()

        def place(t, carry, g=g):
            e = t // slots
            s = t % slots
            index = pos_ref[(spot + e) % inner, s]
            found = index < cap
            lines = held[g][jnp.where(found, index, 0)]
            stage[g][e, s] = jnp.where(found, lines, 0.0)
            return carry

        lax.fori_loop(0, inner * slots, place, 0)
        source = mate(d) * inner + spot
        for e in range(1, inner):
            copy = pltpu.make_async_remote_copy(
                src_ref=stage[g].at[e],
                dst_ref=outs[f].at[:, source],
                send_sem=is_sem.at[g * inner + e],
                recv_sem=ir_sem.at[g * inner + e],
                device_id=peer(plane, (spot + e) % inner),
                device_id_type=pl.DeviceIdType.MESH,
            )
            copy.start()
            near.append(copy)
        copy = pltpu.make_async_copy(stage[g].at[0], outs[f].at[:, source], self_sem.at[g])
        copy.start()
        near.append(copy)
    kept_sums.wait()
    for copy in sums_near:
        copy.wait()
    sums_across = [
        small(by_spot, by_group.at[g], planes + inner + g, (me, (core + g) % groups))
        for g in range(1, groups)
    ]
    oc_ref[core] = jnp.sum(by_spot[...], axis=(0, 1))
    for g in range(1, groups):
        sums_across[g - 1].wait()
        oc_ref[(core + groups - g) % groups] = jnp.sum(by_group[g], axis=(0, 1))
    for f in range(2):
        for d in range(1, planes):
            far[f * planes + d].wait_send()
    for copy in near:
        copy.wait()


def exchange(planes, inner, groups, slots, cap, branch, positions, sums, master_send, update_send):
    lines, lanes = master_send.shape[2:]
    shape = jax.ShapeDtypeStruct((slots, planes * inner, lines, lanes), jnp.float32)
    any_space = pl.BlockSpec(memory_space=pl.ANY)
    steps = 2 * planes
    tile = sums.shape
    hops = planes + inner + groups
    sent = (planes - 1) * cap * 2 * lines * lanes * 4
    return pl.pallas_call(
        functools.partial(exchange_kernel, planes, inner, groups, slots, cap),
        out_shape=(shape, shape, jax.ShapeDtypeStruct((groups, *tile), jnp.float32)),
        in_specs=[
            pl.BlockSpec(memory_space=pltpu.SMEM),
            pl.BlockSpec(memory_space=pltpu.VMEM),
            any_space,
            any_space,
        ],
        out_specs=(any_space, any_space, pl.BlockSpec(memory_space=pltpu.VMEM)),
        scratch_shapes=[pltpu.VMEM((cap, lines, lanes), jnp.float32)] * steps
        + [pltpu.VMEM((inner, slots, lines, lanes), jnp.float32)] * steps
        + [
            pltpu.SemaphoreType.DMA((steps,)),
            pltpu.SemaphoreType.DMA((steps,)),
            pltpu.SemaphoreType.DMA((2,)),
            pltpu.SemaphoreType.DMA((steps * inner,)),
            pltpu.SemaphoreType.DMA((steps * inner,)),
            pltpu.SemaphoreType.DMA((steps,)),
            pltpu.VMEM((planes, *tile), jnp.float32),
            pltpu.VMEM((inner, planes, *tile), jnp.float32),
            pltpu.VMEM((groups, inner, planes, *tile), jnp.float32),
            pltpu.SemaphoreType.DMA((hops,)),
            pltpu.SemaphoreType.DMA((hops,)),
            pltpu.SemaphoreType.DMA((2,)),
        ],
        cost_estimate=pl.CostEstimate(flops=0, bytes_accessed=sent * 4, transcendentals=0),
        compiler_params=pltpu.CompilerParams(
            collective_id=branch, has_side_effects=True, vmem_limit_bytes=60 * 1024 * 1024
        ),
    )(positions, sums, master_send, update_send)


def shards_general(number_base, single, master, first_moment, second_moment, rotation, assignment):
    dp_count = lax.axis_size("dp")
    group_count = lax.axis_size("expert")
    position = lax.axis_index("dp")
    round_count = rotation.shape[0]
    rows_here = master.shape[1]
    lane_count = LANE
    per_row = master.shape[2] // lane_count
    lines_device = rows_here * per_row
    piece_len = lines_device // (round_count * dp_count)
    inv_count = 1.0 / math.sqrt(dp_count * piece_len * lane_count)
    table = slot_table(rotation, dp_count, MOST)
    span_count = round_count * dp_count
    inner = INNER
    planes = dp_count // inner
    slots = round_count * MOST

    plane_of = rotation.reshape(span_count) // inner
    span_ids = jnp.arange(span_count, dtype=jnp.int32)
    same = (plane_of[:, None] == plane_of[None, :]) & (span_ids[None, :] < span_ids[:, None])
    place_of = jnp.sum(same.astype(jnp.int32), axis=1)
    plane_ids = jnp.arange(planes, dtype=jnp.int32)
    loads = jnp.sum((plane_of[None, :] == plane_ids[:, None]).astype(jnp.int32), axis=1)
    most_load = jnp.max(loads)
    cap_all = min(inner * slots, span_count)
    mean_load = span_count // planes
    shares = () if single else (10, 11, 12, 13, 14, 16)
    caps = sorted({min(cap_all, mean_load * eighths // 8) for eighths in shares} | {cap_all})
    choice = sum(((most_load > cap).astype(jnp.int32) for cap in caps[:-1]), jnp.int32(0))
    place_ids = jnp.arange(cap_all, dtype=jnp.int32)
    listed = (plane_of[None, None, :] == plane_ids[:, None, None]) & (
        place_of[None, None, :] == place_ids[None, :, None]
    )
    lists = jnp.sum(listed.astype(jnp.int32) * span_ids, axis=2)
    mine = table.transpose(2, 0, 1).reshape(planes, inner, round_count, MOST)
    mine = lax.dynamic_index_in_dim(mine, position // inner, 0, keepdims=False)
    padded_place = jnp.concatenate(
        [place_of.reshape(round_count, dp_count), jnp.full((round_count, 1), cap_all, jnp.int32)], axis=1
    )
    hits = mine[..., None] == jnp.arange(dp_count + 1, dtype=jnp.int32)
    positions = jnp.sum(hits * padded_place[None, :, None, :], axis=3).reshape(inner, slots)

    update = scaled_moment(first_moment, second_moment)
    master_lines = master.reshape(span_count, piece_len, lane_count)
    update_lines = update.reshape(span_count, piece_len, lane_count)
    local_lines = position * lines_device + jnp.arange(lines_device, dtype=jnp.int32).reshape(
        span_count, piece_len
    )
    weights = position_weights(local_lines, per_row, lane_count)
    master_sums = jnp.sum(master_lines * weights, axis=(1, 2)) * inv_count
    update_sums = jnp.sum(update_lines * weights, axis=(1, 2)) * inv_count

    permuting = (assignment[:, None] == span_ids[None, :]).astype(jnp.float32)
    both_sums = jnp.stack([master_sums, update_sums])
    placed_sums = jnp.sum(both_sums[:, :, None] * permuting[None], axis=1)
    entries = 2 * span_count
    tile_size = 8 * lane_count
    sums = jnp.pad(placed_sums.reshape(entries), (0, -entries % tile_size)).reshape(-1, lane_count)

    def branch_of(number, cap):
        def run(master_in, update_in):
            chosen = lists[:, :cap]
            return exchange(
                planes,
                inner,
                group_count,
                slots,
                cap,
                number_base + number,
                positions,
                sums,
                master_in[chosen],
                update_in[chosen],
            )

        return run

    saved_master, saved_update, totals = lax.switch(
        choice, [branch_of(number, cap) for number, cap in enumerate(caps)], master_lines, update_lines
    )
    checksums = totals.reshape(group_count, -1)[:, :entries].reshape(group_count, 2, span_count)
    shape_out = (1, round_count, MOST, dp_count * piece_len, lane_count)
    return (saved_master.reshape(shape_out), saved_update.reshape(shape_out), checksums)


def layout_of(spans, slots):
    first = 2 * spans
    last = first + 6 * 2 * slots
    spare = last + 16 * slots
    return first, last, spare, -(-(spare + 1) // 128) * 128


def table_kernel(spans, dp_count, most_slots, slots, books, rot_ref, tab_ref, choice_ref, planes_ref, cols_ref, writers_ref, fill_ref, colfill_ref):
    first, last, spare, size = layout_of(spans, slots)
    me = lax.axis_index("dp")
    z, y, x = me // 4, (me // 2) % 2, me % 2
    half = z // 2
    mate = z + 1 - 2 * (z % 2)
    column = 2 * slots

    def clear(i, carry):
        for u in range(8):
            tab_ref[i * 8 + u] = 0
        return carry

    lax.fori_loop(0, last // 8, clear, 0)

    def clear_last(i, carry):
        for u in range(8):
            tab_ref[last + i * 8 + u] = -1
        return carry

    lax.fori_loop(0, 2 * slots, clear_last, 0)
    for p in range(4):
        planes_ref[p] = 0
        fill_ref[p] = 0
    for p in range(16):
        colfill_ref[p] = 0

    def count(r, carry):
        for j in range(dp_count):
            w = rot_ref[r, 0, j]
            planes_ref[w // 4] = planes_ref[w // 4] + 1
        return carry

    lax.fori_loop(0, spans // dp_count, count, 0)

    def one_round(r, carry):
        for p in range(dp_count):
            writers_ref[p] = 0

        def one_span(j, inner_carry):
            c = r * dp_count + j
            w = rot_ref[r, 0, j]
            wz, wy, wx = w // 4, (w // 2) % 2, w % 2
            k = writers_ref[w]
            writers_ref[w] = k + 1
            in_plane = fill_ref[wz]
            fill_ref[wz] = in_plane + 1
            near = ((wz + 1) // 2) % 2
            outer = (wz // 2) * 3
            in_half = in_plane + near * planes_ref[outer]
            tab_ref[jnp.where(wz // 2 != half, in_half, spare)] = c
            tab_ref[jnp.where(wz == mate, spans + in_plane, spare)] = c
            in_cols = []
            for a in range(2):
                spot = wz * 4 + a * 2 + (wy if a else wx)
                in_cols.append(colfill_ref[spot])
                colfill_ref[spot] = in_cols[a] + 1

            @pl.when(wz == z)
            def _():
                q = r * most_slots + k
                for a in range(2):
                    away = (wy != y) if a else (wx != x)
                    base = first + a * 3 * column + in_cols[a]
                    for kind, value in enumerate((c, in_plane, in_half)):
                        tab_ref[jnp.where(away, base + kind * column, spare)] = value
                    who = jnp.where((wx == x) if a else (wy == y), 0, 1)
                    base = last + (a * 2 + who) * 4 * slots + q
                    for kind, value in enumerate((c, in_plane, in_half, in_cols[a])):
                        tab_ref[jnp.where(away, spare, base + kind * slots)] = value

            return inner_carry

        lax.fori_loop(0, dp_count, one_span, 0)
        return carry

    lax.fori_loop(0, spans // dp_count, one_round, 0)
    low = planes_ref[0] + planes_ref[1]
    most_half = jnp.maximum(low, spans - low)
    most_plane = planes_ref[0]
    for p in range(1, 4):
        most_plane = jnp.maximum(most_plane, planes_ref[p])
    most_col = colfill_ref[0]
    for p in range(1, 16):
        most_col = jnp.maximum(most_col, colfill_ref[p])
    choice = jnp.int32(len(books))
    for number in reversed(range(len(books))):
        cap_half, cap_plane, cap_col = books[number]
        fits = (most_half <= cap_half) & (most_plane <= cap_plane) & (most_col <= cap_col)
        choice = jnp.where(fits, number, choice)
    choice_ref[0] = choice


def tables_of(rotation, dp_count, slots, books):
    spans = rotation.shape[0] * dp_count
    size = layout_of(spans, slots)[3]
    smem = pl.BlockSpec(memory_space=pltpu.SMEM)
    return pl.pallas_call(
        functools.partial(table_kernel, spans, dp_count, MOST, slots, books),
        out_shape=(jax.ShapeDtypeStruct((size,), jnp.int32), jax.ShapeDtypeStruct((1,), jnp.int32)),
        in_specs=[smem],
        out_specs=(smem, smem),
        scratch_shapes=[
            pltpu.SMEM((4,), jnp.int32),
            pltpu.SMEM((1,), jnp.int32),
            pltpu.SMEM((dp_count,), jnp.int32),
            pltpu.SMEM((4,), jnp.int32),
            pltpu.SMEM((16,), jnp.int32),
        ],
    )(rotation.transpose(0, 2, 1))


def fast_kernel(
    spans, slots, parts, lines, groups, inv_count, cap_half, cap_plane, cap_col,
    tab, asg_ref, wt_ref, m_ref, a_ref, b_ref, out_ref, oc_ref,
    raw_m, raw_a, raw_b, fld, xs, zs, lz, lc, fs, lf, bs, ss, work, rows_ref, sums, sums_in, across,
    load_sem, xs_sem, lc_sem, zs_sem, lz_sem, fw_sem, fs_sem, lf_sem, bs_sem, out_sem, ss_sem, cs_sem, cr_sem,
):
    first, last, _, _ = layout_of(spans, slots)
    column = 2 * slots
    steps = 2 * parts
    ring = parts
    me = lax.axis_index("dp")
    core = lax.axis_index("expert")
    z, y, x = me // 4, (me // 2) % 2, me % 2
    spot = me % 4
    inner = (z == 1) | (z == 2)
    outer = (z == 0) | (z == 3)
    outer_int = ((z + 1) // 2 + 1) % 2
    mate_x = me + 1 - 2 * x
    mate_y = me + 2 - 4 * y
    z_one = z + 1 - 2 * (z % 2)
    z_two = z + 2 - 4 * (z // 2)
    z_three = 3 - z
    mate_z = z_one * 4 + spot
    cross_to = (2 - z // 2) * 4 + spot
    plane_of = (
        z,
        z_one,
        z_two + outer_int * (z_three - z_two),
        z_three + outer_int * (z_two - z_three),
    )

    def to(dp_index):
        return (dp_index, core)

    def remote(src, dst, send, recv, target):
        return pltpu.make_async_remote_copy(
            src_ref=src,
            dst_ref=dst,
            send_sem=send,
            recv_sem=recv,
            device_id=target,
            device_id_type=pl.DeviceIdType.MESH,
        )

    loads = [
        pltpu.make_async_copy(ref, raw, load_sem.at[n])
        for n, (ref, raw) in enumerate(((m_ref, raw_m), (a_ref, raw_a), (b_ref, raw_b)))
    ]
    for copy in loads:
        copy.start()
    barrier = pltpu.get_barrier_semaphore()
    for target in (mate_x, mate_y, mate_z, z_two * 4 + spot, z_three * 4 + spot):
        pl.semaphore_signal(barrier, inc=1, device_id=to(target), device_id_type=pl.DeviceIdType.MESH)
    for g in range(1, groups):
        pl.semaphore_signal(
            barrier, inc=1, device_id=(me, (core + g) % groups), device_id_type=pl.DeviceIdType.MESH
        )
    pl.semaphore_wait(barrier, 4 + groups)

    def relay(raw, k):
        i = k % parts

        def step(c, carry):
            row = c * parts + i
            start = (row // 8) * (8 * lines) + row % 8
            fld[k, c] = raw[pl.ds(start, lines, stride=8), :]
            return carry

        lax.fori_loop(0, spans, step, 0)

    def pick(count, base, load, store):
        def step(t, carry):
            for u in range(2):
                store(2 * t + u, load(tab[base + 2 * t + u]))
            return carry

        lax.fori_loop(0, count // 2, step, 0)
        if count % 2:
            store(count - 1, load(tab[base + count - 1]))

    def load_from(j, k):
        if j == 0:
            return lambda n: fld[k, n]
        return lambda n: work[n]

    def take(count, *at):
        ref = at[0]

        def step(t, carry):
            for u in range(2):
                work[2 * t + u] = ref[(*at[1:], 2 * t + u)]
            return carry

        lax.fori_loop(0, count // 2, step, 0)
        if count % 2:
            work[count - 1] = ref[(*at[1:], count - 1)]

    def cross_copy(k):
        return remote(
            xs.at[k], lc.at[1 - outer_int, k], xs_sem.at[k], lc_sem.at[1 - outer_int, k], to(cross_to)
        )

    def plane_copy(k):
        return remote(zs.at[k], lz.at[k], zs_sem.at[k], lz_sem.at[k], to(mate_z))

    def forward_copy(s, k):
        return remote(
            lc.at[s, k, pl.ds(0, cap_plane)],
            lc.at[s, k, pl.ds(0, cap_plane)],
            fw_sem.at[s, k],
            lc_sem.at[s, k],
            to(mate_z),
        )

    def first_copy(j, k):
        a = k % 2
        return remote(
            fs.at[k % ring, j], lf.at[k, j], fs_sem.at[k % ring, j], lf_sem.at[k, j], to(mate_x + a * (mate_y - mate_x))
        )

    def last_copy(n, k, own):
        a = k % 2
        if n < 4:
            source = plane_of[n] * 4 + spot
        else:
            source = plane_of[n - 4] * 4 + mate_x % 4 + a * (mate_y - mate_x)
        place = out_ref.at[k // parts, :, source, pl.ds((k % parts) * lines, lines)]
        if own:
            return pltpu.make_async_copy(ss.at[n, k % 2], place, ss_sem.at[n, k % 2])
        return remote(
            bs.at[k % ring, n], place, bs_sem.at[k % ring, n], out_sem.at[k], to(mate_y + a * (mate_x - mate_y))
        )

    def first_hop(j, k):
        kind = min(j, 2)
        copy = first_copy(j, k)

        @pl.when(k >= ring)
        def _():
            copy.wait_send()

        def store(t, value):
            fs[k % ring, j, t] = value

        pick(cap_col, first + ((k % 2) * 3 + kind) * column, load_from(j, k), store)
        copy.start()

    def last_hop(n, k):
        kind = min(n, 2) if n < 4 else 3
        load = load_from(n, k)
        across_copy, own_copy = last_copy(n, k, False), last_copy(n, k, True)

        @pl.when(k >= ring)
        def _():
            across_copy.wait_send()

        base = last + ((k % 2) * 2 + 1) * 4 * slots + kind * slots
        for q in range(slots):
            index = tab[base + q]
            found = index >= 0
            value = load(jnp.where(found, index, 0))
            bs[k % ring, n, q] = jnp.where(found, value, 0.0)
        across_copy.start()

        @pl.when(k >= 2)
        def _():
            own_copy.wait()

        base = last + (k % 2) * 2 * 4 * slots + kind * slots
        for q in range(slots):
            index = tab[base + q]
            found = index >= 0
            value = load(jnp.where(found, index, 0))
            ss[n, k % 2, q] = jnp.where(found, value, 0.0)
        own_copy.start()

    def own_list(raw):
        def step(k, carry):
            relay(raw, k)

            def store_x(t, value):
                xs[k, t] = value

            def store_z(t, value):
                zs[k, t] = value

            pick(cap_half, 0, load_from(0, k), store_x)
            cross_copy(k).start()
            pick(cap_plane, spans, load_from(0, k), store_z)
            plane_copy(k).start()
            first_hop(0, k)
            last_hop(0, k)
            return carry

        return step

    loads[0].wait()
    lax.fori_loop(0, parts, own_list(raw_m), 0)
    loads[1].wait()
    loads[2].wait()
    corr_one = 1.0 - BETA_ONE**STEP
    corr_two = 1.0 - BETA_TWO**STEP

    def moments(t, carry):
        at = pl.ds(t * 64, 64)
        raw_a[at, :] = raw_a[at, :] / corr_one / (jnp.sqrt(raw_b[at, :] / corr_two) + EPSILON)
        return carry

    lax.fori_loop(0, raw_a.shape[0] // 64, moments, 0)
    lax.fori_loop(parts, steps, own_list(raw_a), 0)

    sums[0] = jnp.zeros(sums.shape[1:], jnp.float32)
    for f in range(2):
        def one_piece(c, carry, f=f):
            total = jnp.zeros(fld.shape[2:], jnp.float32)
            for i in range(parts):
                row = (me * spans + c) * parts + i
                total = total + fld[f * parts + i, c] * wt_ref[(row * 5) % 11]
            rows_ref[pl.ds(c, 1), :] = jnp.sum(total, axis=0, keepdims=True)
            return carry

        lax.fori_loop(0, spans, one_piece, 0)
        per_span = jnp.sum(rows_ref[...], axis=1, keepdims=True) * inv_count
        rows_ref[...] = jnp.broadcast_to(per_span, rows_ref.shape)
        slot_of = lax.broadcasted_iota(jnp.int32, (1, rows_ref.shape[1]), 1)

        def one_place(c, placed):
            return placed + jnp.where(slot_of == asg_ref[c], rows_ref[pl.ds(c, 1), :], 0.0)

        sums[0, pl.ds(f, 1), :] = lax.fori_loop(0, spans, one_place, jnp.zeros(slot_of.shape, jnp.float32))

    turns = (mate_x, mate_y, mate_z, z_two * 4 + spot)

    def turn_copy(t):
        return remote(sums.at[t], sums_in.at[t], cs_sem.at[t], cr_sem.at[t], to(turns[t]))

    def turn_end(t):
        turn_copy(t).wait()
        sums[t + 1] = sums[t] + sums_in[t]

    turn_copy(0).start()

    def sums_at(k, base):
        for t in range(3):
            @pl.when(k == base + 3 * t)
            def _(t=t):
                turn_end(t)
                turn_copy(t + 1).start()

    def near_list(j, k):
        first_copy(j, k).wait_recv()
        take(cap_col, lf, k, j)
        last_hop(4 + j, k)

    def both_hops(j, k):
        first_hop(j, k)
        last_hop(j, k)

    @pl.when(inner)
    def _():
        def step(k, carry):
            near_list(0, k)
            plane_copy(k).wait_recv()
            take(cap_plane, lz, k)
            both_hops(1, k)
            for s in (1, 0):
                remote(xs.at[k], lc.at[s, k], xs_sem.at[k], lc_sem.at[s, k], to(cross_to)).wait_recv()
                forward_copy(s, k).start()
                take(cap_half, lc, s, k)
                both_hops(2 + s, k)

            @pl.when(k >= 1)
            def _():
                for j in (1, 3, 2):
                    near_list(j, k - 1)

            sums_at(k, 4)
            return carry

        lax.fori_loop(0, steps, step, 0)

        for j in (1, 3, 2):
            near_list(j, steps - 1)

        def drain(k, carry):
            for s in range(2):
                forward_copy(s, k).wait_send()
            return carry

        lax.fori_loop(0, steps, drain, 0)

    @pl.when(outer)
    def _():
        def step_near(k, carry):
            plane_copy(k).wait_recv()
            take(cap_plane, lz, k)
            both_hops(1, k)
            near_list(0, k)
            return carry

        lax.fori_loop(0, steps, step_near, 0)

        def step(k, carry):
            near_list(1, k)
            for s in (1, 0):
                forward_copy(s, k).wait_recv()
                take(cap_plane, lc, s, k)
                both_hops(2 + s, k)

            @pl.when(k >= 1)
            def _():
                for j in (3, 2):
                    near_list(j, k - 1)

            sums_at(k, 2)
            return carry

        lax.fori_loop(0, steps, step, 0)
        for j in (3, 2):
            near_list(j, steps - 1)

    turn_end(3)
    sent_across = []
    for g in range(1, groups):
        copy = remote(sums.at[4], across.at[g], cs_sem.at[3 + g], cr_sem.at[3 + g], (me, (core + g) % groups))
        copy.start()
        sent_across.append(copy)

    def finish(k, carry):
        cross_copy(k).wait_send()
        plane_copy(k).wait_send()
        pltpu.make_async_copy(
            out_ref.at[k // parts, :, pl.ds(0, 8), pl.ds((k % parts) * lines, lines)],
            out_ref.at[k // parts, :, pl.ds(0, 8), pl.ds((k % parts) * lines, lines)],
            out_sem.at[k],
        ).wait()
        return carry

    lax.fori_loop(0, steps, finish, 0)

    def finish_ring(k, carry):
        for j in range(4):
            first_copy(j, k).wait_send()
        for n in range(8):
            last_copy(n, k, False).wait_send()
        return carry

    lax.fori_loop(steps - ring, steps, finish_ring, 0)

    def finish_own(k, carry):
        for n in range(8):
            last_copy(n, k, True).wait()
        return carry

    lax.fori_loop(steps - 2, steps, finish_own, 0)
    oc_ref[core] = sums[4]
    for g in range(1, groups):
        sent_across[g - 1].wait()
        oc_ref[(core + groups - g) % groups] = across[g]


def fast_exchange(number, book, slots, spans, parts, lines, lanes, groups, inv_count, tab, places, weights, m_in, a_in, b_in):
    cap_half, cap_plane, cap_col = book
    steps = 2 * parts
    ring = parts
    dp_count = 16 if spans is None else lax.axis_size("dp")
    any_space = pl.BlockSpec(memory_space=pl.ANY)
    vmem = pl.BlockSpec(memory_space=pltpu.VMEM)
    smem = pl.BlockSpec(memory_space=pltpu.SMEM)

    def pieces(*lead):
        return pltpu.VMEM((*lead, lines, lanes), jnp.float32)

    def sems(*lead):
        return pltpu.SemaphoreType.DMA(lead)

    raw = pltpu.VMEM(m_in.shape, jnp.float32)
    return pl.pallas_call(
        functools.partial(fast_kernel, spans, slots, parts, lines, groups, inv_count, cap_half, cap_plane, cap_col),
        out_shape=(
            jax.ShapeDtypeStruct((2, slots, dp_count, parts * lines, lanes), jnp.float32),
            jax.ShapeDtypeStruct((groups, 8, lanes), jnp.float32),
        ),
        in_specs=[smem, smem, vmem, any_space, any_space, any_space],
        out_specs=(any_space, vmem),
        scratch_shapes=[
            raw,
            raw,
            raw,
            pieces(steps, spans),
            pieces(steps, cap_half),
            pieces(steps, cap_plane),
            pieces(steps, cap_plane),
            pieces(2, steps, cap_half),
            pieces(ring, 4, cap_col),
            pieces(steps, 4, cap_col),
            pieces(ring, 8, slots),
            pieces(8, 2, slots),
            pieces(cap_half),
            pltpu.VMEM((spans, lanes), jnp.float32),
            pltpu.VMEM((5, 8, lanes), jnp.float32),
            pltpu.VMEM((4, 8, lanes), jnp.float32),
            pltpu.VMEM((groups, 8, lanes), jnp.float32),
            sems(3),
            sems(steps),
            sems(2, steps),
            sems(steps),
            sems(steps),
            sems(2, steps),
            sems(ring, 4),
            sems(steps, 4),
            sems(ring, 8),
            sems(steps),
            sems(8, 2),
            sems(3 + groups),
            sems(3 + groups),
        ],
        cost_estimate=pl.CostEstimate(flops=0, bytes_accessed=4 * m_in.size * 8, transcendentals=0),
        compiler_params=pltpu.CompilerParams(
            collective_id=number, has_side_effects=True, vmem_limit_bytes=67043328
        ),
    )(tab, places, weights, m_in, a_in, b_in)


def shards(master, first_moment, second_moment, rotation, assignment):
    dp_count = lax.axis_size("dp")
    group_count = lax.axis_size("expert")
    round_count = rotation.shape[0]
    rows_here, columns = master.shape[1:]
    lines = columns // LANE
    span_count = round_count * dp_count
    slots = round_count * MOST
    parts = rows_here // span_count
    if dp_count != INNER * 4 or 8 * lines * (rows_here // 8) * LANE != rows_here * columns or span_count > LANE:
        return shards_general(0, False, master, first_moment, second_moment, rotation, assignment)

    half = span_count // 2
    books = ((half + half // 4, half * 13 // 16, slots + 4), (half + half * 11 // 32, half * 29 // 32, slots + 8))
    inv_count = 1.0 / math.sqrt(dp_count * parts * lines * LANE)
    tab, choice = tables_of(rotation, dp_count, slots, books)
    places = assignment
    pattern = np.arange(11)[:, None] + 3 * np.arange(columns)[None, :]
    weights = (1.0 + (pattern % 11).astype(np.float32) / np.float32(10.0)).astype(np.float32)
    weights = jnp.asarray(weights.reshape(11, lines, LANE))

    def tile_order(array):
        return array.reshape(rows_here // 8, 8, lines, LANE).transpose(0, 2, 1, 3).reshape(rows_here * lines, LANE)

    def fast(number, book):
        def run(tab_in, master_in, first_in, second_in):
            saved, totals = fast_exchange(
                number, book, slots, span_count, parts, lines, LANE, group_count, inv_count,
                tab_in, places, weights, tile_order(master_in), tile_order(first_in), tile_order(second_in),
            )
            return saved, totals[:, :2, :span_count]

        return run

    def general(tab_in, master_in, first_in, second_in):
        kept = shards_general(len(books), True, master_in, first_in, second_in, rotation, assignment)
        both = [saved.reshape(slots, dp_count, parts * lines, LANE) for saved in kept[:2]]
        return jnp.stack(both), kept[2]

    branches = [fast(number, book) for number, book in enumerate(books)] + [general]
    saved, checksums = lax.switch(choice[0], branches, tab, master, first_moment, second_moment)
    shape_out = (1, round_count, MOST, dp_count * parts * lines, LANE)
    return saved[0].reshape(shape_out), saved[1].reshape(shape_out), checksums


def solution(mesh):
    placed = (P("expert", "dp", None), P("expert", "dp", None), P("expert", "dp", None), P(), P())
    return jax.shard_map(
        shards,
        mesh=mesh,
        in_specs=placed,
        out_specs=(P("expert", "dp", None, None, None), P("expert", "dp", None, None, None), P()),
        check_vma=False,
    )
```

```python
import functools
import math

import jax
import jax.numpy as jnp
import numpy as np
from jax import lax
from jax.experimental import pallas as pl
from jax.experimental.pallas import tpu as pltpu
from jax.sharding import PartitionSpec as P

LANE = 128
MOST = 3
STEP = 20
INNER = 4


BETA_ONE = 0.9
BETA_TWO = 0.95
EPSILON = 1e-08


def scaled_moment(first_part, second_part):
    corr_one = 1.0 - BETA_ONE**STEP
    corr_two = 1.0 - BETA_TWO**STEP
    return first_part / corr_one / (jnp.sqrt(second_part / corr_two) + EPSILON)


def slot_table(rotation, dp_count, most_slots):
    owners = rotation[:, :, 0]
    span_ids = jnp.arange(dp_count, dtype=jnp.int32)
    same_writer = owners[:, :, None] == owners[:, None, :]
    before = span_ids[None, :] < span_ids[:, None]
    slot_rank = jnp.sum((same_writer & before[None]).astype(jnp.int32), axis=2)
    writers = jnp.arange(dp_count, dtype=jnp.int32)
    slot_ids = jnp.arange(most_slots, dtype=jnp.int32)
    matches = (owners[:, None, None, :] == writers[None, None, :, None]) & (
        slot_rank[:, None, None, :] == slot_ids[None, :, None, None]
    )
    matches = matches.astype(jnp.int32)
    found_any = jnp.sum(matches, axis=3)
    picked = jnp.sum(matches * span_ids, axis=3)
    return picked + (1 - found_any) * dp_count


def position_weights(line_ids, per_row, lane_count):
    row_ids = line_ids // per_row
    col_ids = line_ids % per_row * lane_count
    lane_ids = jnp.arange(lane_count, dtype=jnp.int32)
    pattern = (row_ids[..., None] * 5 + (col_ids[..., None] + lane_ids) * 3) % 11
    return 1.0 + pattern.astype(jnp.float32) / 10.0


def exchange_kernel(
    planes, inner, groups, slots, cap, pos_ref, sum_ref, m_ref, u_ref, om_ref, ou_ref, oc_ref, *scratch
):
    held = scratch[: 2 * planes]
    stage = scratch[2 * planes : 4 * planes]
    zs_sem, zr_sem, local_sem, is_sem, ir_sem, self_sem = scratch[4 * planes : 4 * planes + 6]
    by_plane, by_spot, by_group, cs_sem, cr_sem, cl_sem = scratch[4 * planes + 6 :]
    me = lax.axis_index("dp")
    plane = me // inner
    spot = me % inner
    core = lax.axis_index("expert")
    fields = (m_ref, u_ref)
    outs = (om_ref, ou_ref)

    def peer(plane_to, spot_to):
        return (plane_to * inner + spot_to, core)

    def mate(d):
        other, bit = plane, 1
        while bit < planes:
            if d & bit:
                other = other + bit * (1 - 2 * ((plane // bit) % 2))
            bit *= 2
        return other

    barrier = pltpu.get_barrier_semaphore()
    for d in range(1, planes):
        pl.semaphore_signal(
            barrier, inc=1, device_id=peer(mate(d), spot), device_id_type=pl.DeviceIdType.MESH
        )
    for e in range(1, inner):
        pl.semaphore_signal(
            barrier, inc=1, device_id=peer(plane, (spot + e) % inner), device_id_type=pl.DeviceIdType.MESH
        )
    for g in range(1, groups):
        pl.semaphore_signal(
            barrier, inc=1, device_id=(me, (core + g) % groups), device_id_type=pl.DeviceIdType.MESH
        )
    pl.semaphore_wait(barrier, planes + inner + groups - 3)

    def small(src, dst, number, to):
        copy = pltpu.make_async_remote_copy(
            src_ref=src,
            dst_ref=dst,
            send_sem=cs_sem.at[number],
            recv_sem=cr_sem.at[number],
            device_id=to,
            device_id_type=pl.DeviceIdType.MESH,
        )
        copy.start()
        return copy

    own_sums = pltpu.make_async_copy(sum_ref, by_plane.at[0], cl_sem.at[0])
    own_sums.start()
    sums_far = [
        small(sum_ref, by_plane.at[d], d, peer(mate(d), spot)) for d in range(1, planes)
    ]

    far = [None] * (2 * planes)
    for f in range(2):
        own = pltpu.make_async_copy(fields[f].at[plane], held[f * planes], local_sem.at[f])
        own.start()
        far[f * planes] = own
        for d in range(1, planes):
            to_plane = mate(d)
            copy = pltpu.make_async_remote_copy(
                src_ref=fields[f].at[to_plane],
                dst_ref=held[f * planes + d],
                send_sem=zs_sem.at[f * planes + d],
                recv_sem=zr_sem.at[f * planes + d],
                device_id=peer(to_plane, spot),
                device_id_type=pl.DeviceIdType.MESH,
            )
            copy.start()
            far[f * planes + d] = copy

    own_sums.wait()
    for copy in sums_far:
        copy.wait()
    kept_sums = pltpu.make_async_copy(by_plane, by_spot.at[0], cl_sem.at[1])
    kept_sums.start()
    sums_near = [
        small(by_plane, by_spot.at[e], planes + e, peer(plane, (spot + e) % inner)) for e in range(1, inner)
    ]

    near = []
    order = [(f, 0) for f in range(2)] + [(f, d) for f in range(2) for d in range(1, planes)]
    for f, d in order:
        g = f * planes + d
        if d == 0:
            far[g].wait()
        else:
            far[g].wait_recv()

        def place(t, carry, g=g):
            e = t // slots
            s = t % slots
            index = pos_ref[(spot + e) % inner, s]
            found = index < cap
            lines = held[g][jnp.where(found, index, 0)]
            stage[g][e, s] = jnp.where(found, lines, 0.0)
            return carry

        lax.fori_loop(0, inner * slots, place, 0)
        source = mate(d) * inner + spot
        for e in range(1, inner):
            copy = pltpu.make_async_remote_copy(
                src_ref=stage[g].at[e],
                dst_ref=outs[f].at[:, source],
                send_sem=is_sem.at[g * inner + e],
                recv_sem=ir_sem.at[g * inner + e],
                device_id=peer(plane, (spot + e) % inner),
                device_id_type=pl.DeviceIdType.MESH,
            )
            copy.start()
            near.append(copy)
        copy = pltpu.make_async_copy(stage[g].at[0], outs[f].at[:, source], self_sem.at[g])
        copy.start()
        near.append(copy)
    kept_sums.wait()
    for copy in sums_near:
        copy.wait()
    sums_across = [
        small(by_spot, by_group.at[g], planes + inner + g, (me, (core + g) % groups))
        for g in range(1, groups)
    ]
    oc_ref[core] = jnp.sum(by_spot[...], axis=(0, 1))
    for g in range(1, groups):
        sums_across[g - 1].wait()
        oc_ref[(core + groups - g) % groups] = jnp.sum(by_group[g], axis=(0, 1))
    for f in range(2):
        for d in range(1, planes):
            far[f * planes + d].wait_send()
    for copy in near:
        copy.wait()


def exchange(planes, inner, groups, slots, cap, branch, positions, sums, master_send, update_send):
    lines, lanes = master_send.shape[2:]
    shape = jax.ShapeDtypeStruct((slots, planes * inner, lines, lanes), jnp.float32)
    any_space = pl.BlockSpec(memory_space=pl.ANY)
    steps = 2 * planes
    tile = sums.shape
    hops = planes + inner + groups
    sent = (planes - 1) * cap * 2 * lines * lanes * 4
    return pl.pallas_call(
        functools.partial(exchange_kernel, planes, inner, groups, slots, cap),
        out_shape=(shape, shape, jax.ShapeDtypeStruct((groups, *tile), jnp.float32)),
        in_specs=[
            pl.BlockSpec(memory_space=pltpu.SMEM),
            pl.BlockSpec(memory_space=pltpu.VMEM),
            any_space,
            any_space,
        ],
        out_specs=(any_space, any_space, pl.BlockSpec(memory_space=pltpu.VMEM)),
        scratch_shapes=[pltpu.VMEM((cap, lines, lanes), jnp.float32)] * steps
        + [pltpu.VMEM((inner, slots, lines, lanes), jnp.float32)] * steps
        + [
            pltpu.SemaphoreType.DMA((steps,)),
            pltpu.SemaphoreType.DMA((steps,)),
            pltpu.SemaphoreType.DMA((2,)),
            pltpu.SemaphoreType.DMA((steps * inner,)),
            pltpu.SemaphoreType.DMA((steps * inner,)),
            pltpu.SemaphoreType.DMA((steps,)),
            pltpu.VMEM((planes, *tile), jnp.float32),
            pltpu.VMEM((inner, planes, *tile), jnp.float32),
            pltpu.VMEM((groups, inner, planes, *tile), jnp.float32),
            pltpu.SemaphoreType.DMA((hops,)),
            pltpu.SemaphoreType.DMA((hops,)),
            pltpu.SemaphoreType.DMA((2,)),
        ],
        cost_estimate=pl.CostEstimate(flops=0, bytes_accessed=sent * 4, transcendentals=0),
        compiler_params=pltpu.CompilerParams(
            collective_id=branch, has_side_effects=True, vmem_limit_bytes=60 * 1024 * 1024
        ),
    )(positions, sums, master_send, update_send)


def shards_general(number_base, single, master, first_moment, second_moment, rotation, assignment):
    dp_count = lax.axis_size("dp")
    group_count = lax.axis_size("expert")
    position = lax.axis_index("dp")
    round_count = rotation.shape[0]
    rows_here = master.shape[1]
    lane_count = LANE
    per_row = master.shape[2] // lane_count
    lines_device = rows_here * per_row
    piece_len = lines_device // (round_count * dp_count)
    inv_count = 1.0 / math.sqrt(dp_count * piece_len * lane_count)
    table = slot_table(rotation, dp_count, MOST)
    span_count = round_count * dp_count
    inner = INNER
    planes = dp_count // inner
    slots = round_count * MOST

    plane_of = rotation.reshape(span_count) // inner
    span_ids = jnp.arange(span_count, dtype=jnp.int32)
    same = (plane_of[:, None] == plane_of[None, :]) & (span_ids[None, :] < span_ids[:, None])
    place_of = jnp.sum(same.astype(jnp.int32), axis=1)
    plane_ids = jnp.arange(planes, dtype=jnp.int32)
    loads = jnp.sum((plane_of[None, :] == plane_ids[:, None]).astype(jnp.int32), axis=1)
    most_load = jnp.max(loads)
    cap_all = min(inner * slots, span_count)
    mean_load = span_count // planes
    shares = () if single else (10, 11, 12, 13, 14, 16)
    caps = sorted({min(cap_all, mean_load * eighths // 8) for eighths in shares} | {cap_all})
    choice = sum(((most_load > cap).astype(jnp.int32) for cap in caps[:-1]), jnp.int32(0))
    place_ids = jnp.arange(cap_all, dtype=jnp.int32)
    listed = (plane_of[None, None, :] == plane_ids[:, None, None]) & (
        place_of[None, None, :] == place_ids[None, :, None]
    )
    lists = jnp.sum(listed.astype(jnp.int32) * span_ids, axis=2)
    mine = table.transpose(2, 0, 1).reshape(planes, inner, round_count, MOST)
    mine = lax.dynamic_index_in_dim(mine, position // inner, 0, keepdims=False)
    padded_place = jnp.concatenate(
        [place_of.reshape(round_count, dp_count), jnp.full((round_count, 1), cap_all, jnp.int32)], axis=1
    )
    hits = mine[..., None] == jnp.arange(dp_count + 1, dtype=jnp.int32)
    positions = jnp.sum(hits * padded_place[None, :, None, :], axis=3).reshape(inner, slots)

    update = scaled_moment(first_moment, second_moment)
    master_lines = master.reshape(span_count, piece_len, lane_count)
    update_lines = update.reshape(span_count, piece_len, lane_count)
    local_lines = position * lines_device + jnp.arange(lines_device, dtype=jnp.int32).reshape(
        span_count, piece_len
    )
    weights = position_weights(local_lines, per_row, lane_count)
    master_sums = jnp.sum(master_lines * weights, axis=(1, 2)) * inv_count
    update_sums = jnp.sum(update_lines * weights, axis=(1, 2)) * inv_count

    permuting = (assignment[:, None] == span_ids[None, :]).astype(jnp.float32)
    both_sums = jnp.stack([master_sums, update_sums])
    placed_sums = jnp.sum(both_sums[:, :, None] * permuting[None], axis=1)
    entries = 2 * span_count
    tile_size = 8 * lane_count
    sums = jnp.pad(placed_sums.reshape(entries), (0, -entries % tile_size)).reshape(-1, lane_count)

    def branch_of(number, cap):
        def run(master_in, update_in):
            chosen = lists[:, :cap]
            return exchange(
                planes,
                inner,
                group_count,
                slots,
                cap,
                number_base + number,
                positions,
                sums,
                master_in[chosen],
                update_in[chosen],
            )

        return run

    saved_master, saved_update, totals = lax.switch(
        choice, [branch_of(number, cap) for number, cap in enumerate(caps)], master_lines, update_lines
    )
    checksums = totals.reshape(group_count, -1)[:, :entries].reshape(group_count, 2, span_count)
    shape_out = (1, round_count, MOST, dp_count * piece_len, lane_count)
    return (saved_master.reshape(shape_out), saved_update.reshape(shape_out), checksums)


def layout_of(spans, slots):
    first = 2 * spans
    last = first + 6 * 2 * slots
    spare = last + 16 * slots
    return first, last, spare, -(-(spare + 1) // 128) * 128


def table_kernel(spans, dp_count, most_slots, slots, books, rot_ref, tab_ref, choice_ref, planes_ref, cols_ref, writers_ref, fill_ref, colfill_ref):
    first, last, spare, size = layout_of(spans, slots)
    me = lax.axis_index("dp")
    z, y, x = me // 4, (me // 2) % 2, me % 2
    half = z // 2
    mate = z + 1 - 2 * (z % 2)
    column = 2 * slots

    def clear(i, carry):
        for u in range(8):
            tab_ref[i * 8 + u] = 0
        return carry

    lax.fori_loop(0, last // 8, clear, 0)

    def clear_last(i, carry):
        for u in range(8):
            tab_ref[last + i * 8 + u] = -1
        return carry

    lax.fori_loop(0, 2 * slots, clear_last, 0)
    for p in range(4):
        planes_ref[p] = 0
        fill_ref[p] = 0
    for p in range(16):
        colfill_ref[p] = 0

    def count(r, carry):
        for j in range(dp_count):
            w = rot_ref[r, 0, j]
            planes_ref[w // 4] = planes_ref[w // 4] + 1
        return carry

    lax.fori_loop(0, spans // dp_count, count, 0)

    def one_round(r, carry):
        for p in range(dp_count):
            writers_ref[p] = 0

        def one_span(j, inner_carry):
            c = r * dp_count + j
            w = rot_ref[r, 0, j]
            wz, wy, wx = w // 4, (w // 2) % 2, w % 2
            k = writers_ref[w]
            writers_ref[w] = k + 1
            in_plane = fill_ref[wz]
            fill_ref[wz] = in_plane + 1
            near = ((wz + 1) // 2) % 2
            outer = (wz // 2) * 3
            in_half = in_plane + near * planes_ref[outer]
            tab_ref[jnp.where(wz // 2 != half, in_half, spare)] = c
            tab_ref[jnp.where(wz == mate, spans + in_plane, spare)] = c
            in_cols = []
            for a in range(2):
                spot = wz * 4 + a * 2 + (wy if a else wx)
                in_cols.append(colfill_ref[spot])
                colfill_ref[spot] = in_cols[a] + 1

            @pl.when(wz == z)
            def _():
                q = r * most_slots + k
                for a in range(2):
                    away = (wy != y) if a else (wx != x)
                    base = first + a * 3 * column + in_cols[a]
                    for kind, value in enumerate((c, in_plane, in_half)):
                        tab_ref[jnp.where(away, base + kind * column, spare)] = value
                    who = jnp.where((wx == x) if a else (wy == y), 0, 1)
                    base = last + (a * 2 + who) * 4 * slots + q
                    for kind, value in enumerate((c, in_plane, in_half, in_cols[a])):
                        tab_ref[jnp.where(away, spare, base + kind * slots)] = value

            return inner_carry

        lax.fori_loop(0, dp_count, one_span, 0)
        return carry

    lax.fori_loop(0, spans // dp_count, one_round, 0)
    low = planes_ref[0] + planes_ref[1]
    most_half = jnp.maximum(low, spans - low)
    most_plane = planes_ref[0]
    for p in range(1, 4):
        most_plane = jnp.maximum(most_plane, planes_ref[p])
    most_col = colfill_ref[0]
    for p in range(1, 16):
        most_col = jnp.maximum(most_col, colfill_ref[p])
    choice = jnp.int32(len(books))
    for number in reversed(range(len(books))):
        cap_half, cap_plane, cap_col = books[number]
        fits = (most_half <= cap_half) & (most_plane <= cap_plane) & (most_col <= cap_col)
        choice = jnp.where(fits, number, choice)
    choice_ref[0] = choice


def tables_of(rotation, dp_count, slots, books):
    spans = rotation.shape[0] * dp_count
    size = layout_of(spans, slots)[3]
    smem = pl.BlockSpec(memory_space=pltpu.SMEM)
    return pl.pallas_call(
        functools.partial(table_kernel, spans, dp_count, MOST, slots, books),
        out_shape=(jax.ShapeDtypeStruct((size,), jnp.int32), jax.ShapeDtypeStruct((1,), jnp.int32)),
        in_specs=[smem],
        out_specs=(smem, smem),
        scratch_shapes=[
            pltpu.SMEM((4,), jnp.int32),
            pltpu.SMEM((1,), jnp.int32),
            pltpu.SMEM((dp_count,), jnp.int32),
            pltpu.SMEM((4,), jnp.int32),
            pltpu.SMEM((16,), jnp.int32),
        ],
    )(rotation.transpose(0, 2, 1))


def fast_kernel(
    spans, slots, parts, lines, groups, inv_count, cap_half, cap_plane, cap_col,
    tab, asg_ref, wt_ref, m_ref, a_ref, b_ref, out_ref, oc_ref,
    raw_m, raw_a, raw_b, fld, xs, zs, lz, lc, fs, lf, bs, ss, work, rows_ref, sums, sums_in, across,
    load_sem, xs_sem, lc_sem, zs_sem, lz_sem, fw_sem, fs_sem, lf_sem, bs_sem, out_sem, ss_sem, cs_sem, cr_sem,
):
    first, last, _, _ = layout_of(spans, slots)
    column = 2 * slots
    steps = 2 * parts
    ring = parts
    me = lax.axis_index("dp")
    core = lax.axis_index("expert")
    z, y, x = me // 4, (me // 2) % 2, me % 2
    spot = me % 4
    inner = (z == 1) | (z == 2)
    outer = (z == 0) | (z == 3)
    outer_int = ((z + 1) // 2 + 1) % 2
    mate_x = me + 1 - 2 * x
    mate_y = me + 2 - 4 * y
    z_one = z + 1 - 2 * (z % 2)
    z_two = z + 2 - 4 * (z // 2)
    z_three = 3 - z
    mate_z = z_one * 4 + spot
    cross_to = (2 - z // 2) * 4 + spot
    plane_of = (
        z,
        z_one,
        z_two + outer_int * (z_three - z_two),
        z_three + outer_int * (z_two - z_three),
    )

    def to(dp_index):
        return (dp_index, core)

    def remote(src, dst, send, recv, target):
        return pltpu.make_async_remote_copy(
            src_ref=src,
            dst_ref=dst,
            send_sem=send,
            recv_sem=recv,
            device_id=target,
            device_id_type=pl.DeviceIdType.MESH,
        )

    loads = [
        pltpu.make_async_copy(ref, raw, load_sem.at[n])
        for n, (ref, raw) in enumerate(((m_ref, raw_m), (a_ref, raw_a), (b_ref, raw_b)))
    ]
    loads[0].start()
    barrier = pltpu.get_barrier_semaphore()
    for target in (mate_x, mate_y, mate_z, z_two * 4 + spot, z_three * 4 + spot):
        pl.semaphore_signal(barrier, inc=1, device_id=to(target), device_id_type=pl.DeviceIdType.MESH)
    for g in range(1, groups):
        pl.semaphore_signal(
            barrier, inc=1, device_id=(me, (core + g) % groups), device_id_type=pl.DeviceIdType.MESH
        )
    pl.semaphore_wait(barrier, 4 + groups)

    def relay(raw, k):
        i = k % parts

        def step(c, carry):
            row = c * parts + i
            start = (row // 8) * (8 * lines) + row % 8
            fld[k, c] = raw[pl.ds(start, lines, stride=8), :]
            return carry

        lax.fori_loop(0, spans, step, 0)

    def pick(count, base, load, store):
        def step(t, carry):
            for u in range(2):
                store(2 * t + u, load(tab[base + 2 * t + u]))
            return carry

        lax.fori_loop(0, count // 2, step, 0)
        if count % 2:
            store(count - 1, load(tab[base + count - 1]))

    def load_from(j, k):
        if j == 0:
            return lambda n: fld[k, n]
        return lambda n: work[n]

    def take(count, *at):
        ref = at[0]

        def step(t, carry):
            for u in range(2):
                work[2 * t + u] = ref[(*at[1:], 2 * t + u)]
            return carry

        lax.fori_loop(0, count // 2, step, 0)
        if count % 2:
            work[count - 1] = ref[(*at[1:], count - 1)]

    def cross_copy(k):
        return remote(
            xs.at[k], lc.at[1 - outer_int, k], xs_sem.at[k], lc_sem.at[1 - outer_int, k], to(cross_to)
        )

    def plane_copy(k):
        return remote(zs.at[k], lz.at[k], zs_sem.at[k], lz_sem.at[k], to(mate_z))

    def forward_copy(s, k):
        return remote(
            lc.at[s, k, pl.ds(0, cap_plane)],
            lc.at[s, k, pl.ds(0, cap_plane)],
            fw_sem.at[s, k],
            lc_sem.at[s, k],
            to(mate_z),
        )

    def first_copy(j, k):
        a = k % 2
        return remote(
            fs.at[k % ring, j], lf.at[k, j], fs_sem.at[k % ring, j], lf_sem.at[k, j], to(mate_x + a * (mate_y - mate_x))
        )

    def last_copy(n, k, own):
        a = k % 2
        if n < 4:
            source = plane_of[n] * 4 + spot
        else:
            source = plane_of[n - 4] * 4 + mate_x % 4 + a * (mate_y - mate_x)
        place = out_ref.at[k // parts, :, source, pl.ds((k % parts) * lines, lines)]
        if own:
            return pltpu.make_async_copy(ss.at[n, k % 2], place, ss_sem.at[n, k % 2])
        return remote(
            bs.at[k % ring, n], place, bs_sem.at[k % ring, n], out_sem.at[k], to(mate_y + a * (mate_x - mate_y))
        )

    def first_hop(j, k):
        kind = min(j, 2)
        copy = first_copy(j, k)

        @pl.when(k >= ring)
        def _():
            copy.wait_send()

        def store(t, value):
            fs[k % ring, j, t] = value

        pick(cap_col, first + ((k % 2) * 3 + kind) * column, load_from(j, k), store)
        copy.start()

    def last_hop(n, k):
        kind = min(n, 2) if n < 4 else 3
        load = load_from(n, k)
        across_copy, own_copy = last_copy(n, k, False), last_copy(n, k, True)

        @pl.when(k >= ring)
        def _():
            across_copy.wait_send()

        base = last + ((k % 2) * 2 + 1) * 4 * slots + kind * slots
        for q in range(slots):
            index = tab[base + q]
            found = index >= 0
            value = load(jnp.where(found, index, 0))
            bs[k % ring, n, q] = jnp.where(found, value, 0.0)
        across_copy.start()

        @pl.when(k >= 2)
        def _():
            own_copy.wait()

        base = last + (k % 2) * 2 * 4 * slots + kind * slots
        for q in range(slots):
            index = tab[base + q]
            found = index >= 0
            value = load(jnp.where(found, index, 0))
            ss[n, k % 2, q] = jnp.where(found, value, 0.0)
        own_copy.start()

    def own_list(raw):
        def step(k, carry):
            relay(raw, k)

            def store_x(t, value):
                xs[k, t] = value

            def store_z(t, value):
                zs[k, t] = value

            pick(cap_half, 0, load_from(0, k), store_x)
            cross_copy(k).start()

            @pl.when(inner)
            def _():
                pick(cap_plane, spans, load_from(0, k), store_z)
                plane_copy(k).start()

            first_hop(0, k)
            last_hop(0, k)
            return carry

        return step

    loads[0].wait()
    loads[1].start()
    loads[2].start()
    lax.fori_loop(0, parts, own_list(raw_m), 0)
    loads[1].wait()
    loads[2].wait()
    corr_one = 1.0 - BETA_ONE**STEP
    corr_two = 1.0 - BETA_TWO**STEP

    def moments(t, carry):
        at = pl.ds(t * 64, 64)
        raw_a[at, :] = raw_a[at, :] * (1.0 / corr_one) / (jnp.sqrt(raw_b[at, :] * (1.0 / corr_two)) + EPSILON)
        return carry

    lax.fori_loop(0, raw_a.shape[0] // 64, moments, 0)
    lax.fori_loop(parts, steps, own_list(raw_a), 0)

    @pl.when(outer)
    def _():
        def step(k, carry):
            def store_z(t, value):
                zs[k, t] = value

            pick(cap_plane, spans, load_from(0, k), store_z)
            plane_copy(k).start()
            return carry

        lax.fori_loop(0, steps, step, 0)

    sums[0] = jnp.zeros(sums.shape[1:], jnp.float32)
    for f in range(2):
        def one_piece(c, carry, f=f):
            total = jnp.zeros(fld.shape[2:], jnp.float32)
            for i in range(parts):
                row = (me * spans + c) * parts + i
                total = total + fld[f * parts + i, c] * wt_ref[(row * 5) % 11]
            rows_ref[pl.ds(c, 1), :] = jnp.sum(total, axis=0, keepdims=True)
            return carry

        lax.fori_loop(0, spans, one_piece, 0)
        per_span = jnp.sum(rows_ref[...], axis=1, keepdims=True) * inv_count
        rows_ref[...] = jnp.broadcast_to(per_span, rows_ref.shape)
        slot_of = lax.broadcasted_iota(jnp.int32, (1, rows_ref.shape[1]), 1)

        def one_place(c, placed):
            return placed + jnp.where(slot_of == asg_ref[c], rows_ref[pl.ds(c, 1), :], 0.0)

        sums[0, pl.ds(f, 1), :] = lax.fori_loop(0, spans, one_place, jnp.zeros(slot_of.shape, jnp.float32))

    turns = (mate_x, mate_y, mate_z, z_two * 4 + spot)

    def turn_copy(t):
        return remote(sums.at[t], sums_in.at[t], cs_sem.at[t], cr_sem.at[t], to(turns[t]))

    def turn_end(t):
        turn_copy(t).wait()
        sums[t + 1] = sums[t] + sums_in[t]

    turn_copy(0).start()

    def sums_at(k, base):
        for t in range(3):
            @pl.when(k == base + 3 * t)
            def _(t=t):
                turn_end(t)
                turn_copy(t + 1).start()

    def near_list(j, k):
        first_copy(j, k).wait_recv()
        take(cap_col, lf, k, j)
        last_hop(4 + j, k)

    def both_hops(j, k):
        first_hop(j, k)
        last_hop(j, k)

    def after_first(j, k):
        @pl.when(k >= 1)
        def _():
            near_list(j, k - 1)

    @pl.when(inner)
    def _():
        def crossed(s, k):
            remote(xs.at[k], lc.at[s, k], xs_sem.at[k], lc_sem.at[s, k], to(cross_to)).wait_recv()
            forward_copy(s, k).start()
            take(cap_half, lc, s, k)
            both_hops(2 + s, k)

        def step(k, carry):
            near_list(0, k)
            crossed(0, k)
            after_first(2, k)
            return carry

        lax.fori_loop(0, steps, step, 0)
        near_list(2, steps - 1)

        def step_far(k, carry):
            plane_copy(k).wait_recv()
            take(cap_plane, lz, k)
            both_hops(1, k)
            crossed(1, k)
            after_first(1, k)
            after_first(3, k)
            sums_at(k, 1)
            return carry

        lax.fori_loop(0, steps, step_far, 0)
        near_list(1, steps - 1)
        near_list(3, steps - 1)

        def drain(k, carry):
            for s in range(2):
                forward_copy(s, k).wait_send()
            return carry

        lax.fori_loop(0, steps, drain, 0)

    @pl.when(outer)
    def _():
        def step_near(k, carry):
            plane_copy(k).wait_recv()
            take(cap_plane, lz, k)
            both_hops(1, k)
            near_list(0, k)
            return carry

        lax.fori_loop(0, steps, step_near, 0)

        def forwarded(s, k):
            forward_copy(s, k).wait_recv()
            take(cap_plane, lc, s, k)
            both_hops(2 + s, k)

        def step(k, carry):
            forwarded(0, k)
            near_list(1, k)
            after_first(2, k)
            return carry

        lax.fori_loop(0, steps, step, 0)
        near_list(2, steps - 1)

        def step_far(k, carry):
            forwarded(1, k)
            after_first(3, k)
            sums_at(k, 1)
            return carry

        lax.fori_loop(0, steps, step_far, 0)
        near_list(3, steps - 1)

    turn_end(3)
    sent_across = []
    for g in range(1, groups):
        copy = remote(sums.at[4], across.at[g], cs_sem.at[3 + g], cr_sem.at[3 + g], (me, (core + g) % groups))
        copy.start()
        sent_across.append(copy)

    def finish(k, carry):
        cross_copy(k).wait_send()
        plane_copy(k).wait_send()
        pltpu.make_async_copy(
            out_ref.at[k // parts, :, pl.ds(0, 8), pl.ds((k % parts) * lines, lines)],
            out_ref.at[k // parts, :, pl.ds(0, 8), pl.ds((k % parts) * lines, lines)],
            out_sem.at[k],
        ).wait()
        return carry

    lax.fori_loop(0, steps, finish, 0)

    def finish_ring(k, carry):
        for j in range(4):
            first_copy(j, k).wait_send()
        for n in range(8):
            last_copy(n, k, False).wait_send()
        return carry

    lax.fori_loop(steps - ring, steps, finish_ring, 0)

    def finish_own(k, carry):
        for n in range(8):
            last_copy(n, k, True).wait()
        return carry

    lax.fori_loop(steps - 2, steps, finish_own, 0)
    oc_ref[core] = sums[4]
    for g in range(1, groups):
        sent_across[g - 1].wait()
        oc_ref[(core + groups - g) % groups] = across[g]


def fast_exchange(number, book, slots, spans, parts, lines, lanes, groups, inv_count, tab, places, weights, m_in, a_in, b_in):
    cap_half, cap_plane, cap_col = book
    steps = 2 * parts
    ring = parts
    dp_count = 16 if spans is None else lax.axis_size("dp")
    any_space = pl.BlockSpec(memory_space=pl.ANY)
    vmem = pl.BlockSpec(memory_space=pltpu.VMEM)
    smem = pl.BlockSpec(memory_space=pltpu.SMEM)

    def pieces(*lead):
        return pltpu.VMEM((*lead, lines, lanes), jnp.float32)

    def sems(*lead):
        return pltpu.SemaphoreType.DMA(lead)

    raw = pltpu.VMEM(m_in.shape, jnp.float32)
    return pl.pallas_call(
        functools.partial(fast_kernel, spans, slots, parts, lines, groups, inv_count, cap_half, cap_plane, cap_col),
        out_shape=(
            jax.ShapeDtypeStruct((2, slots, dp_count, parts * lines, lanes), jnp.float32),
            jax.ShapeDtypeStruct((groups, 8, lanes), jnp.float32),
        ),
        in_specs=[smem, smem, vmem, any_space, any_space, any_space],
        out_specs=(any_space, vmem),
        scratch_shapes=[
            raw,
            raw,
            raw,
            pieces(steps, spans),
            pieces(steps, cap_half),
            pieces(steps, cap_plane),
            pieces(steps, cap_plane),
            pieces(2, steps, cap_half),
            pieces(ring, 4, cap_col),
            pieces(steps, 4, cap_col),
            pieces(ring, 8, slots),
            pieces(8, 2, slots),
            pieces(cap_half),
            pltpu.VMEM((spans, lanes), jnp.float32),
            pltpu.VMEM((5, 8, lanes), jnp.float32),
            pltpu.VMEM((4, 8, lanes), jnp.float32),
            pltpu.VMEM((groups, 8, lanes), jnp.float32),
            sems(3),
            sems(steps),
            sems(2, steps),
            sems(steps),
            sems(steps),
            sems(2, steps),
            sems(ring, 4),
            sems(steps, 4),
            sems(ring, 8),
            sems(steps),
            sems(8, 2),
            sems(3 + groups),
            sems(3 + groups),
        ],
        cost_estimate=pl.CostEstimate(flops=0, bytes_accessed=4 * m_in.size * 8, transcendentals=0),
        compiler_params=pltpu.CompilerParams(
            collective_id=number, has_side_effects=True, vmem_limit_bytes=67043328
        ),
    )(tab, places, weights, m_in, a_in, b_in)


def shards(master, first_moment, second_moment, rotation, assignment):
    dp_count = lax.axis_size("dp")
    group_count = lax.axis_size("expert")
    round_count = rotation.shape[0]
    rows_here, columns = master.shape[1:]
    lines = columns // LANE
    span_count = round_count * dp_count
    slots = round_count * MOST
    parts = rows_here // span_count
    if dp_count != INNER * 4 or 8 * lines * (rows_here // 8) * LANE != rows_here * columns or span_count > LANE:
        return shards_general(0, False, master, first_moment, second_moment, rotation, assignment)

    half = span_count // 2
    books = ((half + half // 4, half * 13 // 16, slots + 4), (half + half * 11 // 32, half * 29 // 32, slots + 8))
    inv_count = 1.0 / math.sqrt(dp_count * parts * lines * LANE)
    tab, choice = tables_of(rotation, dp_count, slots, books)
    places = assignment
    pattern = np.arange(11)[:, None] + 3 * np.arange(columns)[None, :]
    weights = (1.0 + (pattern % 11).astype(np.float32) / np.float32(10.0)).astype(np.float32)
    weights = jnp.asarray(weights.reshape(11, lines, LANE))

    def tile_order(array):
        return array.reshape(rows_here // 8, 8, lines, LANE).transpose(0, 2, 1, 3).reshape(rows_here * lines, LANE)

    def fast(number, book):
        def run(tab_in, master_in, first_in, second_in):
            saved, totals = fast_exchange(
                number, book, slots, span_count, parts, lines, LANE, group_count, inv_count,
                tab_in, places, weights, tile_order(master_in), tile_order(first_in), tile_order(second_in),
            )
            return saved, totals[:, :2, :span_count]

        return run

    def general(tab_in, master_in, first_in, second_in):
        kept = shards_general(len(books), True, master_in, first_in, second_in, rotation, assignment)
        both = [saved.reshape(slots, dp_count, parts * lines, LANE) for saved in kept[:2]]
        return jnp.stack(both), kept[2]

    branches = [fast(number, book) for number, book in enumerate(books)] + [general]
    saved, checksums = lax.switch(choice[0], branches, tab, master, first_moment, second_moment)
    shape_out = (1, round_count, MOST, dp_count * parts * lines, LANE)
    return saved[0].reshape(shape_out), saved[1].reshape(shape_out), checksums


def solution(mesh):
    placed = (P("expert", "dp", None), P("expert", "dp", None), P("expert", "dp", None), P(), P())
    return jax.shard_map(
        shards,
        mesh=mesh,
        in_specs=placed,
        out_specs=(P("expert", "dp", None, None, None), P("expert", "dp", None, None, None), P()),
        check_vma=False,
    )
```

```python
import functools
import math

import jax
import jax.numpy as jnp
import numpy as np
from jax import lax
from jax.experimental import pallas as pl
from jax.experimental.pallas import tpu as pltpu
from jax.sharding import PartitionSpec as P

LANE = 128
MOST = 3
STEP = 20
INNER = 4


BETA_ONE = 0.9
BETA_TWO = 0.95
EPSILON = 1e-08


def scaled_moment(first_part, second_part):
    corr_one = 1.0 - BETA_ONE**STEP
    corr_two = 1.0 - BETA_TWO**STEP
    return first_part / corr_one / (jnp.sqrt(second_part / corr_two) + EPSILON)


def slot_table(rotation, dp_count, most_slots):
    owners = rotation[:, :, 0]
    span_ids = jnp.arange(dp_count, dtype=jnp.int32)
    same_writer = owners[:, :, None] == owners[:, None, :]
    before = span_ids[None, :] < span_ids[:, None]
    slot_rank = jnp.sum((same_writer & before[None]).astype(jnp.int32), axis=2)
    writers = jnp.arange(dp_count, dtype=jnp.int32)
    slot_ids = jnp.arange(most_slots, dtype=jnp.int32)
    matches = (owners[:, None, None, :] == writers[None, None, :, None]) & (
        slot_rank[:, None, None, :] == slot_ids[None, :, None, None]
    )
    matches = matches.astype(jnp.int32)
    found_any = jnp.sum(matches, axis=3)
    picked = jnp.sum(matches * span_ids, axis=3)
    return picked + (1 - found_any) * dp_count


def position_weights(line_ids, per_row, lane_count):
    row_ids = line_ids // per_row
    col_ids = line_ids % per_row * lane_count
    lane_ids = jnp.arange(lane_count, dtype=jnp.int32)
    pattern = (row_ids[..., None] * 5 + (col_ids[..., None] + lane_ids) * 3) % 11
    return 1.0 + pattern.astype(jnp.float32) / 10.0


def exchange_kernel(
    planes, inner, groups, slots, cap, pos_ref, sum_ref, m_ref, u_ref, om_ref, ou_ref, oc_ref, *scratch
):
    held = scratch[: 2 * planes]
    stage = scratch[2 * planes : 4 * planes]
    zs_sem, zr_sem, local_sem, is_sem, ir_sem, self_sem = scratch[4 * planes : 4 * planes + 6]
    by_plane, by_spot, by_group, cs_sem, cr_sem, cl_sem = scratch[4 * planes + 6 :]
    me = lax.axis_index("dp")
    plane = me // inner
    spot = me % inner
    core = lax.axis_index("expert")
    fields = (m_ref, u_ref)
    outs = (om_ref, ou_ref)

    def peer(plane_to, spot_to):
        return (plane_to * inner + spot_to, core)

    def mate(d):
        other, bit = plane, 1
        while bit < planes:
            if d & bit:
                other = other + bit * (1 - 2 * ((plane // bit) % 2))
            bit *= 2
        return other

    barrier = pltpu.get_barrier_semaphore()
    for d in range(1, planes):
        pl.semaphore_signal(
            barrier, inc=1, device_id=peer(mate(d), spot), device_id_type=pl.DeviceIdType.MESH
        )
    for e in range(1, inner):
        pl.semaphore_signal(
            barrier, inc=1, device_id=peer(plane, (spot + e) % inner), device_id_type=pl.DeviceIdType.MESH
        )
    for g in range(1, groups):
        pl.semaphore_signal(
            barrier, inc=1, device_id=(me, (core + g) % groups), device_id_type=pl.DeviceIdType.MESH
        )
    pl.semaphore_wait(barrier, planes + inner + groups - 3)

    def small(src, dst, number, to):
        copy = pltpu.make_async_remote_copy(
            src_ref=src,
            dst_ref=dst,
            send_sem=cs_sem.at[number],
            recv_sem=cr_sem.at[number],
            device_id=to,
            device_id_type=pl.DeviceIdType.MESH,
        )
        copy.start()
        return copy

    own_sums = pltpu.make_async_copy(sum_ref, by_plane.at[0], cl_sem.at[0])
    own_sums.start()
    sums_far = [
        small(sum_ref, by_plane.at[d], d, peer(mate(d), spot)) for d in range(1, planes)
    ]

    far = [None] * (2 * planes)
    for f in range(2):
        own = pltpu.make_async_copy(fields[f].at[plane], held[f * planes], local_sem.at[f])
        own.start()
        far[f * planes] = own
        for d in range(1, planes):
            to_plane = mate(d)
            copy = pltpu.make_async_remote_copy(
                src_ref=fields[f].at[to_plane],
                dst_ref=held[f * planes + d],
                send_sem=zs_sem.at[f * planes + d],
                recv_sem=zr_sem.at[f * planes + d],
                device_id=peer(to_plane, spot),
                device_id_type=pl.DeviceIdType.MESH,
            )
            copy.start()
            far[f * planes + d] = copy

    own_sums.wait()
    for copy in sums_far:
        copy.wait()
    kept_sums = pltpu.make_async_copy(by_plane, by_spot.at[0], cl_sem.at[1])
    kept_sums.start()
    sums_near = [
        small(by_plane, by_spot.at[e], planes + e, peer(plane, (spot + e) % inner)) for e in range(1, inner)
    ]

    near = []
    order = [(f, 0) for f in range(2)] + [(f, d) for f in range(2) for d in range(1, planes)]
    for f, d in order:
        g = f * planes + d
        if d == 0:
            far[g].wait()
        else:
            far[g].wait_recv()

        def place(t, carry, g=g):
            e = t // slots
            s = t % slots
            index = pos_ref[(spot + e) % inner, s]
            found = index < cap
            lines = held[g][jnp.where(found, index, 0)]
            stage[g][e, s] = jnp.where(found, lines, 0.0)
            return carry

        lax.fori_loop(0, inner * slots, place, 0)
        source = mate(d) * inner + spot
        for e in range(1, inner):
            copy = pltpu.make_async_remote_copy(
                src_ref=stage[g].at[e],
                dst_ref=outs[f].at[:, source],
                send_sem=is_sem.at[g * inner + e],
                recv_sem=ir_sem.at[g * inner + e],
                device_id=peer(plane, (spot + e) % inner),
                device_id_type=pl.DeviceIdType.MESH,
            )
            copy.start()
            near.append(copy)
        copy = pltpu.make_async_copy(stage[g].at[0], outs[f].at[:, source], self_sem.at[g])
        copy.start()
        near.append(copy)
    kept_sums.wait()
    for copy in sums_near:
        copy.wait()
    sums_across = [
        small(by_spot, by_group.at[g], planes + inner + g, (me, (core + g) % groups))
        for g in range(1, groups)
    ]
    oc_ref[core] = jnp.sum(by_spot[...], axis=(0, 1))
    for g in range(1, groups):
        sums_across[g - 1].wait()
        oc_ref[(core + groups - g) % groups] = jnp.sum(by_group[g], axis=(0, 1))
    for f in range(2):
        for d in range(1, planes):
            far[f * planes + d].wait_send()
    for copy in near:
        copy.wait()


def exchange(planes, inner, groups, slots, cap, branch, positions, sums, master_send, update_send):
    lines, lanes = master_send.shape[2:]
    shape = jax.ShapeDtypeStruct((slots, planes * inner, lines, lanes), jnp.float32)
    any_space = pl.BlockSpec(memory_space=pl.ANY)
    steps = 2 * planes
    tile = sums.shape
    hops = planes + inner + groups
    sent = (planes - 1) * cap * 2 * lines * lanes * 4
    return pl.pallas_call(
        functools.partial(exchange_kernel, planes, inner, groups, slots, cap),
        out_shape=(shape, shape, jax.ShapeDtypeStruct((groups, *tile), jnp.float32)),
        in_specs=[
            pl.BlockSpec(memory_space=pltpu.SMEM),
            pl.BlockSpec(memory_space=pltpu.VMEM),
            any_space,
            any_space,
        ],
        out_specs=(any_space, any_space, pl.BlockSpec(memory_space=pltpu.VMEM)),
        scratch_shapes=[pltpu.VMEM((cap, lines, lanes), jnp.float32)] * steps
        + [pltpu.VMEM((inner, slots, lines, lanes), jnp.float32)] * steps
        + [
            pltpu.SemaphoreType.DMA((steps,)),
            pltpu.SemaphoreType.DMA((steps,)),
            pltpu.SemaphoreType.DMA((2,)),
            pltpu.SemaphoreType.DMA((steps * inner,)),
            pltpu.SemaphoreType.DMA((steps * inner,)),
            pltpu.SemaphoreType.DMA((steps,)),
            pltpu.VMEM((planes, *tile), jnp.float32),
            pltpu.VMEM((inner, planes, *tile), jnp.float32),
            pltpu.VMEM((groups, inner, planes, *tile), jnp.float32),
            pltpu.SemaphoreType.DMA((hops,)),
            pltpu.SemaphoreType.DMA((hops,)),
            pltpu.SemaphoreType.DMA((2,)),
        ],
        cost_estimate=pl.CostEstimate(flops=0, bytes_accessed=sent * 4, transcendentals=0),
        compiler_params=pltpu.CompilerParams(
            collective_id=branch, has_side_effects=True, vmem_limit_bytes=60 * 1024 * 1024
        ),
    )(positions, sums, master_send, update_send)


def shards_general(number_base, single, master, first_moment, second_moment, rotation, assignment):
    dp_count = lax.axis_size("dp")
    group_count = lax.axis_size("expert")
    position = lax.axis_index("dp")
    round_count = rotation.shape[0]
    rows_here = master.shape[1]
    lane_count = LANE
    per_row = master.shape[2] // lane_count
    lines_device = rows_here * per_row
    piece_len = lines_device // (round_count * dp_count)
    inv_count = 1.0 / math.sqrt(dp_count * piece_len * lane_count)
    table = slot_table(rotation, dp_count, MOST)
    span_count = round_count * dp_count
    inner = INNER
    planes = dp_count // inner
    slots = round_count * MOST

    plane_of = rotation.reshape(span_count) // inner
    span_ids = jnp.arange(span_count, dtype=jnp.int32)
    same = (plane_of[:, None] == plane_of[None, :]) & (span_ids[None, :] < span_ids[:, None])
    place_of = jnp.sum(same.astype(jnp.int32), axis=1)
    plane_ids = jnp.arange(planes, dtype=jnp.int32)
    loads = jnp.sum((plane_of[None, :] == plane_ids[:, None]).astype(jnp.int32), axis=1)
    most_load = jnp.max(loads)
    cap_all = min(inner * slots, span_count)
    mean_load = span_count // planes
    shares = () if single else (10, 11, 12, 13, 14, 16)
    caps = sorted({min(cap_all, mean_load * eighths // 8) for eighths in shares} | {cap_all})
    choice = sum(((most_load > cap).astype(jnp.int32) for cap in caps[:-1]), jnp.int32(0))
    place_ids = jnp.arange(cap_all, dtype=jnp.int32)
    listed = (plane_of[None, None, :] == plane_ids[:, None, None]) & (
        place_of[None, None, :] == place_ids[None, :, None]
    )
    lists = jnp.sum(listed.astype(jnp.int32) * span_ids, axis=2)
    mine = table.transpose(2, 0, 1).reshape(planes, inner, round_count, MOST)
    mine = lax.dynamic_index_in_dim(mine, position // inner, 0, keepdims=False)
    padded_place = jnp.concatenate(
        [place_of.reshape(round_count, dp_count), jnp.full((round_count, 1), cap_all, jnp.int32)], axis=1
    )
    hits = mine[..., None] == jnp.arange(dp_count + 1, dtype=jnp.int32)
    positions = jnp.sum(hits * padded_place[None, :, None, :], axis=3).reshape(inner, slots)

    update = scaled_moment(first_moment, second_moment)
    master_lines = master.reshape(span_count, piece_len, lane_count)
    update_lines = update.reshape(span_count, piece_len, lane_count)
    local_lines = position * lines_device + jnp.arange(lines_device, dtype=jnp.int32).reshape(
        span_count, piece_len
    )
    weights = position_weights(local_lines, per_row, lane_count)
    master_sums = jnp.sum(master_lines * weights, axis=(1, 2)) * inv_count
    update_sums = jnp.sum(update_lines * weights, axis=(1, 2)) * inv_count

    permuting = (assignment[:, None] == span_ids[None, :]).astype(jnp.float32)
    both_sums = jnp.stack([master_sums, update_sums])
    placed_sums = jnp.sum(both_sums[:, :, None] * permuting[None], axis=1)
    entries = 2 * span_count
    tile_size = 8 * lane_count
    sums = jnp.pad(placed_sums.reshape(entries), (0, -entries % tile_size)).reshape(-1, lane_count)

    def branch_of(number, cap):
        def run(master_in, update_in):
            chosen = lists[:, :cap]
            return exchange(
                planes,
                inner,
                group_count,
                slots,
                cap,
                number_base + number,
                positions,
                sums,
                master_in[chosen],
                update_in[chosen],
            )

        return run

    saved_master, saved_update, totals = lax.switch(
        choice, [branch_of(number, cap) for number, cap in enumerate(caps)], master_lines, update_lines
    )
    checksums = totals.reshape(group_count, -1)[:, :entries].reshape(group_count, 2, span_count)
    shape_out = (1, round_count, MOST, dp_count * piece_len, lane_count)
    return (saved_master.reshape(shape_out), saved_update.reshape(shape_out), checksums)


FIRST = 2
LAST = FIRST + 6
TABLES = LAST + 16


def table_kernel(books, most_slots, rot_ref, tab_ref, choice_ref):
    rounds, _, dp_count = rot_ref.shape
    spans = rounds * dp_count
    me = lax.axis_index("dp")
    z, y, x = me // 4, (me // 2) % 2, me % 2
    mate = z + 1 - 2 * (z % 2)
    lane = lax.broadcasted_iota(jnp.int32, (1, LANE), 1)
    sub = lax.broadcasted_iota(jnp.int32, (8, LANE), 0)
    row = jnp.full((1, LANE), -1, jnp.int32)
    blocks = []
    for c in range(spans):
        if c % 8 == 0:
            block = jnp.zeros((8, LANE), jnp.int32)
        w = rot_ref[c // dp_count, 0, c % dp_count]
        row = jnp.where(lane == c, w, row)
        block = jnp.where(sub == c % 8, w, block)
        if c % 8 == 7:
            blocks.append(block)
    shape = (spans, LANE)
    writer = jnp.concatenate(blocks, axis=0)
    writer_across = jnp.broadcast_to(row, shape)
    span = lax.broadcasted_iota(jnp.int32, shape, 0)
    across = lax.broadcasted_iota(jnp.int32, shape, 1)
    before = across < span

    def rank(same):
        return jnp.sum(jnp.where(same & before, 1.0, 0.0), axis=1, keepdims=True)

    def spread(values):
        return jnp.broadcast_to(values.astype(jnp.int32), shape)

    def plane_of(w):
        return lax.shift_right_arithmetic(w, 2)

    def bit(w, n):
        return lax.shift_right_arithmetic(w, n) & 1

    plane, plane_across = plane_of(writer), plane_of(writer_across)
    same_plane = plane == plane_across
    in_plane_f = rank(same_plane)
    half_f = rank(lax.shift_right_arithmetic(writer, 3) == lax.shift_right_arithmetic(writer_across, 3))
    cols_f = [rank(same_plane & (bit(writer, a) == bit(writer_across, a))) for a in range(2)]
    round_of, round_across = span // dp_count, across // dp_count
    turn = spread(rank((writer == writer_across) & (round_of == round_across)))
    outer = [jnp.sum(jnp.where(plane == p, 1, 0), axis=0, keepdims=True) for p in (0, 3)]
    in_plane = spread(in_plane_f)
    in_half = in_plane + jnp.where(plane == 1, outer[0], 0) + jnp.where(plane == 2, outer[1], 0)
    in_cols = [spread(c) for c in cols_f]
    slot = round_of * most_slots + turn

    def put(number, mask, value, absent):
        picked = jnp.sum(jnp.where(mask, value - absent, 0), axis=0, keepdims=True)
        tab_ref[pl.ds(number, 1), :] = picked + absent

    put(0, (lax.shift_right_arithmetic(writer, 3) != z // 2) & (in_half == across), span, 0)
    put(1, (plane == mate) & (in_plane == across), span, 0)
    here = plane == z
    at_slot = here & (slot == across)
    for a in range(2):
        mine, other = (y, x) if a else (x, y)
        in_col = bit(writer, a) == mine
        mask = here & jnp.logical_not(in_col) & (in_cols[a] == across)
        for kind, value in enumerate((span, in_plane, in_half)):
            put(FIRST + a * 3 + kind, mask, value, 0)
        for who in range(2):
            mask = at_slot & in_col & (bit(writer, 1 - a) == (other if who == 0 else 1 - other))
            for kind, value in enumerate((span, in_plane, in_half, in_cols[a])):
                put(LAST + (a * 2 + who) * 4 + kind, mask, value, -1)
    most_half, most_plane = jnp.max(half_f) + 1.0, jnp.max(in_plane_f) + 1.0
    most_col = jnp.maximum(jnp.max(cols_f[0]), jnp.max(cols_f[1])) + 1.0
    choice = jnp.int32(len(books))
    for number in reversed(range(len(books))):
        cap_half, cap_plane, cap_col = books[number]
        fits = (most_half <= cap_half) & (most_plane <= cap_plane) & (most_col <= cap_col)
        choice = jnp.where(fits, number, choice)
    choice_ref[0] = choice


def tables_of(rotation, books):
    smem = pl.BlockSpec(memory_space=pltpu.SMEM)
    return pl.pallas_call(
        functools.partial(table_kernel, books, MOST),
        out_shape=(jax.ShapeDtypeStruct((TABLES, LANE), jnp.int32), jax.ShapeDtypeStruct((1,), jnp.int32)),
        in_specs=[smem],
        out_specs=(pl.BlockSpec(memory_space=pltpu.VMEM), smem),
    )(rotation.transpose(0, 2, 1))


def deliver_kernel(saved_ref, totals_ref, om_ref, ou_ref, oc_ref, held, in_sem, out_sem):
    slots = om_ref.shape[0]
    takes = []
    for f in range(2):
        for q in range(slots):
            n = f * slots + q
            takes.append(pltpu.make_async_copy(saved_ref.at[f, q], held.at[n], in_sem.at[n]))
            takes[n].start()
    oc_ref[...] = totals_ref[:, : oc_ref.shape[1], : oc_ref.shape[2]]
    gives = []
    for f, out_ref in enumerate((om_ref, ou_ref)):
        for q in range(slots):
            n = f * slots + q
            takes[n].wait()
            gives.append(pltpu.make_async_copy(held.at[n], out_ref.at[q], out_sem.at[n]))
            gives[n].start()
    for give in gives:
        give.wait()


def deliver(saved, totals, spans):
    slots = saved.shape[1]
    any_space = pl.BlockSpec(memory_space=pl.ANY)
    vmem = pl.BlockSpec(memory_space=pltpu.VMEM)
    out = jax.ShapeDtypeStruct(saved.shape[1:], jnp.float32)
    return pl.pallas_call(
        deliver_kernel,
        out_shape=(out, out, jax.ShapeDtypeStruct((totals.shape[0], 2, spans), jnp.float32)),
        in_specs=[any_space, vmem],
        out_specs=(any_space, any_space, vmem),
        scratch_shapes=[
            pltpu.VMEM((2 * slots, *saved.shape[2:]), jnp.float32),
            pltpu.SemaphoreType.DMA((2 * slots,)),
            pltpu.SemaphoreType.DMA((2 * slots,)),
        ],
        cost_estimate=pl.CostEstimate(flops=0, bytes_accessed=saved.size * 8, transcendentals=0),
        compiler_params=pltpu.CompilerParams(vmem_limit_bytes=48 * 1024 * 1024),
    )(saved, totals)


def fast_kernel(
    spans, slots, parts, lines, groups, inv_count, cap_half, cap_plane, cap_col,
    tab, asg_ref, wt_ref, m_ref, a_ref, b_ref, out_ref, oc_ref,
    raw_m, raw_a, raw_b, fld, xs, zs, lz, lc, fs, lf, bs, ss, work, rows_ref, sums, sums_in, across,
    load_sem, xs_sem, lc_sem, zs_sem, lz_sem, fw_sem, fs_sem, lf_sem, bs_sem, out_sem, ss_sem, cs_sem, cr_sem,
):
    steps = 2 * parts
    ring = parts
    me = lax.axis_index("dp")
    core = lax.axis_index("expert")
    z, y, x = me // 4, (me // 2) % 2, me % 2
    spot = me % 4
    inner = (z == 1) | (z == 2)
    outer = (z == 0) | (z == 3)
    outer_int = ((z + 1) // 2 + 1) % 2
    mate_x = me + 1 - 2 * x
    mate_y = me + 2 - 4 * y
    z_one = z + 1 - 2 * (z % 2)
    z_two = z + 2 - 4 * (z // 2)
    z_three = 3 - z
    mate_z = z_one * 4 + spot
    cross_to = (2 - z // 2) * 4 + spot
    plane_of = (
        z,
        z_one,
        z_two + outer_int * (z_three - z_two),
        z_three + outer_int * (z_two - z_three),
    )

    def to(dp_index):
        return (dp_index, core)

    def remote(src, dst, send, recv, target):
        return pltpu.make_async_remote_copy(
            src_ref=src,
            dst_ref=dst,
            send_sem=send,
            recv_sem=recv,
            device_id=target,
            device_id_type=pl.DeviceIdType.MESH,
        )

    loads = [
        pltpu.make_async_copy(ref, raw, load_sem.at[n])
        for n, (ref, raw) in enumerate(((m_ref, raw_m), (a_ref, raw_a), (b_ref, raw_b)))
    ]
    loads[0].start()
    barrier = pltpu.get_barrier_semaphore()
    for target in (mate_x, mate_y, mate_z, z_two * 4 + spot, z_three * 4 + spot):
        pl.semaphore_signal(barrier, inc=1, device_id=to(target), device_id_type=pl.DeviceIdType.MESH)
    for g in range(1, groups):
        pl.semaphore_signal(
            barrier, inc=1, device_id=(me, (core + g) % groups), device_id_type=pl.DeviceIdType.MESH
        )
    pl.semaphore_wait(barrier, 4 + groups)

    def relay(raw, k):
        i = k % parts

        def step(c, carry):
            row = c * parts + i
            start = (row // 8) * (8 * lines) + row % 8
            fld[k, c] = raw[pl.ds(start, lines, stride=8), :]
            return carry

        lax.fori_loop(0, spans, step, 0)

    def pick(count, row, load, store):
        def step(t, carry):
            for u in range(2):
                store(2 * t + u, load(tab[row, 2 * t + u]))
            return carry

        lax.fori_loop(0, count // 2, step, 0)
        if count % 2:
            store(count - 1, load(tab[row, count - 1]))

    def load_from(j, k):
        if j == 0:
            return lambda n: fld[k, n]
        return lambda n: work[n]

    def take(count, *at):
        ref = at[0]

        def step(t, carry):
            for u in range(2):
                work[2 * t + u] = ref[(*at[1:], 2 * t + u)]
            return carry

        lax.fori_loop(0, count // 2, step, 0)
        if count % 2:
            work[count - 1] = ref[(*at[1:], count - 1)]

    def cross_copy(k):
        return remote(
            xs.at[k], lc.at[1 - outer_int, k], xs_sem.at[k], lc_sem.at[1 - outer_int, k], to(cross_to)
        )

    def plane_copy(k):
        return remote(zs.at[k], lz.at[k], zs_sem.at[k], lz_sem.at[k], to(mate_z))

    def forward_copy(s, k):
        return remote(
            lc.at[s, k, pl.ds(0, cap_plane)],
            lc.at[s, k, pl.ds(0, cap_plane)],
            fw_sem.at[s, k],
            lc_sem.at[s, k],
            to(mate_z),
        )

    def first_copy(j, k):
        a = k % 2
        return remote(
            fs.at[k % ring, j], lf.at[k, j], fs_sem.at[k % ring, j], lf_sem.at[k, j], to(mate_x + a * (mate_y - mate_x))
        )

    def last_copy(n, k, own):
        a = k % 2
        if n < 4:
            source = plane_of[n] * 4 + spot
        else:
            source = plane_of[n - 4] * 4 + mate_x % 4 + a * (mate_y - mate_x)
        place = out_ref.at[k // parts, :, source, pl.ds((k % parts) * lines, lines)]
        if own:
            return pltpu.make_async_copy(ss.at[n, k % 2], place, ss_sem.at[n, k % 2])
        return remote(
            bs.at[k % ring, n], place, bs_sem.at[k % ring, n], out_sem.at[k], to(mate_y + a * (mate_x - mate_y))
        )

    def first_hop(j, k):
        kind = min(j, 2)
        copy = first_copy(j, k)

        @pl.when(k >= ring)
        def _():
            copy.wait_send()

        def store(t, value):
            fs[k % ring, j, t] = value

        pick(cap_col, FIRST + (k % 2) * 3 + kind, load_from(j, k), store)
        copy.start()

    def last_hop(n, k):
        kind = min(n, 2) if n < 4 else 3
        load = load_from(n, k)
        across_copy, own_copy = last_copy(n, k, False), last_copy(n, k, True)

        @pl.when(k >= ring)
        def _():
            across_copy.wait_send()

        row = LAST + (k % 2) * 8 + 4 + kind
        for q in range(slots):
            index = tab[row, q]
            found = index >= 0
            value = load(jnp.where(found, index, 0))
            bs[k % ring, n, q] = jnp.where(found, value, 0.0)
        across_copy.start()

        @pl.when(k >= 2)
        def _():
            own_copy.wait()

        row = LAST + (k % 2) * 8 + kind
        for q in range(slots):
            index = tab[row, q]
            found = index >= 0
            value = load(jnp.where(found, index, 0))
            ss[n, k % 2, q] = jnp.where(found, value, 0.0)
        own_copy.start()

    def own_list(raw):
        def step(k, carry):
            relay(raw, k)

            def store_x(t, value):
                xs[k, t] = value

            def store_z(t, value):
                zs[k, t] = value

            pick(cap_half, 0, load_from(0, k), store_x)
            cross_copy(k).start()

            @pl.when(inner)
            def _():
                pick(cap_plane, 1, load_from(0, k), store_z)
                plane_copy(k).start()

            first_hop(0, k)
            last_hop(0, k)
            return carry

        return step

    loads[0].wait()
    loads[1].start()
    loads[2].start()
    lax.fori_loop(0, parts, own_list(raw_m), 0)
    loads[1].wait()
    loads[2].wait()
    corr_one = 1.0 - BETA_ONE**STEP
    corr_two = 1.0 - BETA_TWO**STEP

    def moments(t, carry):
        at = pl.ds(t * 64, 64)
        raw_a[at, :] = raw_a[at, :] * (1.0 / corr_one) / (jnp.sqrt(raw_b[at, :] * (1.0 / corr_two)) + EPSILON)
        return carry

    lax.fori_loop(0, raw_a.shape[0] // 64, moments, 0)
    lax.fori_loop(parts, steps, own_list(raw_a), 0)

    @pl.when(outer)
    def _():
        def step(k, carry):
            def store_z(t, value):
                zs[k, t] = value

            pick(cap_plane, 1, load_from(0, k), store_z)
            plane_copy(k).start()
            return carry

        lax.fori_loop(0, steps, step, 0)

    sums[0] = jnp.zeros(sums.shape[1:], jnp.float32)
    for f in range(2):
        def one_piece(c, carry, f=f):
            total = jnp.zeros(fld.shape[2:], jnp.float32)
            for i in range(parts):
                row = (me * spans + c) * parts + i
                total = total + fld[f * parts + i, c] * wt_ref[(row * 5) % 11]
            rows_ref[pl.ds(c, 1), :] = jnp.sum(total, axis=0, keepdims=True)
            return carry

        lax.fori_loop(0, spans, one_piece, 0)
        per_span = jnp.sum(rows_ref[...], axis=1, keepdims=True) * inv_count
        rows_ref[...] = jnp.broadcast_to(per_span, rows_ref.shape)
        slot_of = lax.broadcasted_iota(jnp.int32, (1, rows_ref.shape[1]), 1)

        def one_place(c, placed):
            return placed + jnp.where(slot_of == asg_ref[c], rows_ref[pl.ds(c, 1), :], 0.0)

        sums[0, pl.ds(f, 1), :] = lax.fori_loop(0, spans, one_place, jnp.zeros(slot_of.shape, jnp.float32))

    turns = (mate_x, mate_y, mate_z, z_two * 4 + spot)

    def turn_copy(t):
        return remote(sums.at[t], sums_in.at[t], cs_sem.at[t], cr_sem.at[t], to(turns[t]))

    def turn_end(t):
        turn_copy(t).wait()
        sums[t + 1] = sums[t] + sums_in[t]

    turn_copy(0).start()

    def sums_at(k, base):
        for t in range(3):
            @pl.when(k == base + 3 * t)
            def _(t=t):
                turn_end(t)
                turn_copy(t + 1).start()

    def near_list(j, k):
        first_copy(j, k).wait_recv()
        take(cap_col, lf, k, j)
        last_hop(4 + j, k)

    def both_hops(j, k):
        first_hop(j, k)
        last_hop(j, k)

    def after_first(j, k):
        @pl.when(k >= 1)
        def _():
            near_list(j, k - 1)

    @pl.when(inner)
    def _():
        def crossed(s, k):
            remote(xs.at[k], lc.at[s, k], xs_sem.at[k], lc_sem.at[s, k], to(cross_to)).wait_recv()
            forward_copy(s, k).start()
            take(cap_half, lc, s, k)
            both_hops(2 + s, k)

        def step(k, carry):
            near_list(0, k)
            crossed(0, k)
            after_first(2, k)
            return carry

        lax.fori_loop(0, steps, step, 0)
        near_list(2, steps - 1)

        def step_far(k, carry):
            plane_copy(k).wait_recv()
            take(cap_plane, lz, k)
            both_hops(1, k)
            crossed(1, k)
            after_first(1, k)
            after_first(3, k)
            sums_at(k, 1)
            return carry

        lax.fori_loop(0, steps, step_far, 0)
        near_list(1, steps - 1)
        near_list(3, steps - 1)

        def drain(k, carry):
            for s in range(2):
                forward_copy(s, k).wait_send()
            return carry

        lax.fori_loop(0, steps, drain, 0)

    @pl.when(outer)
    def _():
        def step_near(k, carry):
            plane_copy(k).wait_recv()
            take(cap_plane, lz, k)
            both_hops(1, k)
            near_list(0, k)
            return carry

        lax.fori_loop(0, steps, step_near, 0)

        def forwarded(s, k):
            forward_copy(s, k).wait_recv()
            take(cap_plane, lc, s, k)
            both_hops(2 + s, k)

        def step(k, carry):
            forwarded(0, k)
            near_list(1, k)
            after_first(2, k)
            return carry

        lax.fori_loop(0, steps, step, 0)
        near_list(2, steps - 1)

        def step_far(k, carry):
            forwarded(1, k)
            after_first(3, k)
            sums_at(k, 1)
            return carry

        lax.fori_loop(0, steps, step_far, 0)
        near_list(3, steps - 1)

    turn_end(3)
    sent_across = []
    for g in range(1, groups):
        copy = remote(sums.at[4], across.at[g], cs_sem.at[3 + g], cr_sem.at[3 + g], (me, (core + g) % groups))
        copy.start()
        sent_across.append(copy)

    def finish(k, carry):
        cross_copy(k).wait_send()
        plane_copy(k).wait_send()
        pltpu.make_async_copy(
            out_ref.at[k // parts, :, pl.ds(0, 8), pl.ds((k % parts) * lines, lines)],
            out_ref.at[k // parts, :, pl.ds(0, 8), pl.ds((k % parts) * lines, lines)],
            out_sem.at[k],
        ).wait()
        return carry

    lax.fori_loop(0, steps, finish, 0)

    def finish_ring(k, carry):
        for j in range(4):
            first_copy(j, k).wait_send()
        for n in range(8):
            last_copy(n, k, False).wait_send()
        return carry

    lax.fori_loop(steps - ring, steps, finish_ring, 0)

    def finish_own(k, carry):
        for n in range(8):
            last_copy(n, k, True).wait()
        return carry

    lax.fori_loop(steps - 2, steps, finish_own, 0)
    oc_ref[core] = sums[4]
    for g in range(1, groups):
        sent_across[g - 1].wait()
        oc_ref[(core + groups - g) % groups] = across[g]


def fast_exchange(number, book, slots, spans, parts, lines, lanes, groups, inv_count, tab, places, weights, m_in, a_in, b_in):
    cap_half, cap_plane, cap_col = book
    steps = 2 * parts
    ring = parts
    dp_count = 16 if spans is None else lax.axis_size("dp")
    any_space = pl.BlockSpec(memory_space=pl.ANY)
    vmem = pl.BlockSpec(memory_space=pltpu.VMEM)
    smem = pl.BlockSpec(memory_space=pltpu.SMEM)

    def pieces(*lead):
        return pltpu.VMEM((*lead, lines, lanes), jnp.float32)

    def sems(*lead):
        return pltpu.SemaphoreType.DMA(lead)

    raw = pltpu.VMEM(m_in.shape, jnp.float32)
    return pl.pallas_call(
        functools.partial(fast_kernel, spans, slots, parts, lines, groups, inv_count, cap_half, cap_plane, cap_col),
        out_shape=(
            jax.ShapeDtypeStruct((2, slots, dp_count, parts * lines, lanes), jnp.float32),
            jax.ShapeDtypeStruct((groups, 8, lanes), jnp.float32),
        ),
        in_specs=[smem, smem, vmem, any_space, any_space, any_space],
        out_specs=(any_space, vmem),
        scratch_shapes=[
            raw,
            raw,
            raw,
            pieces(steps, spans),
            pieces(steps, cap_half),
            pieces(steps, cap_plane),
            pieces(steps, cap_plane),
            pieces(2, steps, cap_half),
            pieces(ring, 4, cap_col),
            pieces(steps, 4, cap_col),
            pieces(ring, 8, slots),
            pieces(8, 2, slots),
            pieces(cap_half),
            pltpu.VMEM((spans, lanes), jnp.float32),
            pltpu.VMEM((5, 8, lanes), jnp.float32),
            pltpu.VMEM((4, 8, lanes), jnp.float32),
            pltpu.VMEM((groups, 8, lanes), jnp.float32),
            sems(3),
            sems(steps),
            sems(2, steps),
            sems(steps),
            sems(steps),
            sems(2, steps),
            sems(ring, 4),
            sems(steps, 4),
            sems(ring, 8),
            sems(steps),
            sems(8, 2),
            sems(3 + groups),
            sems(3 + groups),
        ],
        cost_estimate=pl.CostEstimate(flops=0, bytes_accessed=4 * m_in.size * 8, transcendentals=0),
        compiler_params=pltpu.CompilerParams(
            collective_id=number, has_side_effects=True, vmem_limit_bytes=67043328
        ),
    )(tab, places, weights, m_in, a_in, b_in)


def shards(master, first_moment, second_moment, rotation, assignment):
    dp_count = lax.axis_size("dp")
    group_count = lax.axis_size("expert")
    round_count = rotation.shape[0]
    rows_here, columns = master.shape[1:]
    lines = columns // LANE
    span_count = round_count * dp_count
    slots = round_count * MOST
    parts = rows_here // span_count
    if dp_count != INNER * 4 or 8 * lines * (rows_here // 8) * LANE != rows_here * columns or span_count > LANE:
        return shards_general(0, False, master, first_moment, second_moment, rotation, assignment)

    half = span_count // 2
    books = (
        (half * 9 // 8, half * 3 // 4, slots + 3),
        (half * 19 // 16, half * 13 // 16, slots + 4),
        (half * 5 // 4, half * 27 // 32, slots + 4),
        (half * 11 // 8, half * 29 // 32, slots + 8),
    )
    inv_count = 1.0 / math.sqrt(dp_count * parts * lines * LANE)
    tab, choice = tables_of(rotation, books)
    places = assignment
    pattern = np.arange(11)[:, None] + 3 * np.arange(columns)[None, :]
    weights = (1.0 + (pattern % 11).astype(np.float32) / np.float32(10.0)).astype(np.float32)
    weights = jnp.asarray(weights.reshape(11, lines, LANE))

    def tile_order(array):
        return array.reshape(rows_here // 8, 8, lines, LANE).transpose(0, 2, 1, 3).reshape(rows_here * lines, LANE)

    def fast(number, book):
        def run(tab_in, master_in, first_in, second_in):
            return fast_exchange(
                number, book, slots, span_count, parts, lines, LANE, group_count, inv_count,
                tab_in, places, weights, tile_order(master_in), tile_order(first_in), tile_order(second_in),
            )

        return run

    def general(tab_in, master_in, first_in, second_in):
        kept = shards_general(len(books), True, master_in, first_in, second_in, rotation, assignment)
        both = [saved.reshape(slots, dp_count, parts * lines, LANE) for saved in kept[:2]]
        return jnp.stack(both), jnp.pad(kept[2], ((0, 0), (0, 6), (0, LANE - span_count)))

    branches = [fast(number, book) for number, book in enumerate(books)] + [general]
    saved, totals = lax.switch(choice[0], branches, tab, master, first_moment, second_moment)
    saved_master, saved_update, checksums = deliver(saved, totals, span_count)
    shape_out = (1, round_count, MOST, dp_count * parts * lines, LANE)
    return saved_master.reshape(shape_out), saved_update.reshape(shape_out), checksums


def solution(mesh):
    placed = (P("expert", "dp", None), P("expert", "dp", None), P("expert", "dp", None), P(), P())
    return jax.shard_map(
        shards,
        mesh=mesh,
        in_specs=placed,
        out_specs=(P("expert", "dp", None, None, None), P("expert", "dp", None, None, None), P()),
        check_vma=False,
    )
```

```python
import functools
import math

import jax
import jax.numpy as jnp
import numpy as np
from jax import lax
from jax.experimental import pallas as pl
from jax.experimental.pallas import tpu as pltpu
from jax.sharding import PartitionSpec as P

LANE = 128
MOST = 3
STEP = 20
INNER = 4


BETA_ONE = 0.9
BETA_TWO = 0.95
EPSILON = 1e-08


def scaled_moment(first_part, second_part):
    corr_one = 1.0 - BETA_ONE**STEP
    corr_two = 1.0 - BETA_TWO**STEP
    return first_part / corr_one / (jnp.sqrt(second_part / corr_two) + EPSILON)


def slot_table(rotation, dp_count, most_slots):
    owners = rotation[:, :, 0]
    span_ids = jnp.arange(dp_count, dtype=jnp.int32)
    same_writer = owners[:, :, None] == owners[:, None, :]
    before = span_ids[None, :] < span_ids[:, None]
    slot_rank = jnp.sum((same_writer & before[None]).astype(jnp.int32), axis=2)
    writers = jnp.arange(dp_count, dtype=jnp.int32)
    slot_ids = jnp.arange(most_slots, dtype=jnp.int32)
    matches = (owners[:, None, None, :] == writers[None, None, :, None]) & (
        slot_rank[:, None, None, :] == slot_ids[None, :, None, None]
    )
    matches = matches.astype(jnp.int32)
    found_any = jnp.sum(matches, axis=3)
    picked = jnp.sum(matches * span_ids, axis=3)
    return picked + (1 - found_any) * dp_count


def position_weights(line_ids, per_row, lane_count):
    row_ids = line_ids // per_row
    col_ids = line_ids % per_row * lane_count
    lane_ids = jnp.arange(lane_count, dtype=jnp.int32)
    pattern = (row_ids[..., None] * 5 + (col_ids[..., None] + lane_ids) * 3) % 11
    return 1.0 + pattern.astype(jnp.float32) / 10.0


def exchange_kernel(
    planes, inner, groups, slots, cap, pos_ref, sum_ref, m_ref, u_ref, om_ref, ou_ref, oc_ref, *scratch
):
    held = scratch[: 2 * planes]
    stage = scratch[2 * planes : 4 * planes]
    zs_sem, zr_sem, local_sem, is_sem, ir_sem, self_sem = scratch[4 * planes : 4 * planes + 6]
    by_plane, by_spot, by_group, cs_sem, cr_sem, cl_sem = scratch[4 * planes + 6 :]
    me = lax.axis_index("dp")
    plane = me // inner
    spot = me % inner
    core = lax.axis_index("expert")
    fields = (m_ref, u_ref)
    outs = (om_ref, ou_ref)

    def peer(plane_to, spot_to):
        return (plane_to * inner + spot_to, core)

    def mate(d):
        other, bit = plane, 1
        while bit < planes:
            if d & bit:
                other = other + bit * (1 - 2 * ((plane // bit) % 2))
            bit *= 2
        return other

    barrier = pltpu.get_barrier_semaphore()
    for d in range(1, planes):
        pl.semaphore_signal(
            barrier, inc=1, device_id=peer(mate(d), spot), device_id_type=pl.DeviceIdType.MESH
        )
    for e in range(1, inner):
        pl.semaphore_signal(
            barrier, inc=1, device_id=peer(plane, (spot + e) % inner), device_id_type=pl.DeviceIdType.MESH
        )
    for g in range(1, groups):
        pl.semaphore_signal(
            barrier, inc=1, device_id=(me, (core + g) % groups), device_id_type=pl.DeviceIdType.MESH
        )
    pl.semaphore_wait(barrier, planes + inner + groups - 3)

    def small(src, dst, number, to):
        copy = pltpu.make_async_remote_copy(
            src_ref=src,
            dst_ref=dst,
            send_sem=cs_sem.at[number],
            recv_sem=cr_sem.at[number],
            device_id=to,
            device_id_type=pl.DeviceIdType.MESH,
        )
        copy.start()
        return copy

    own_sums = pltpu.make_async_copy(sum_ref, by_plane.at[0], cl_sem.at[0])
    own_sums.start()
    sums_far = [
        small(sum_ref, by_plane.at[d], d, peer(mate(d), spot)) for d in range(1, planes)
    ]

    far = [None] * (2 * planes)
    for f in range(2):
        own = pltpu.make_async_copy(fields[f].at[plane], held[f * planes], local_sem.at[f])
        own.start()
        far[f * planes] = own
        for d in range(1, planes):
            to_plane = mate(d)
            copy = pltpu.make_async_remote_copy(
                src_ref=fields[f].at[to_plane],
                dst_ref=held[f * planes + d],
                send_sem=zs_sem.at[f * planes + d],
                recv_sem=zr_sem.at[f * planes + d],
                device_id=peer(to_plane, spot),
                device_id_type=pl.DeviceIdType.MESH,
            )
            copy.start()
            far[f * planes + d] = copy

    own_sums.wait()
    for copy in sums_far:
        copy.wait()
    kept_sums = pltpu.make_async_copy(by_plane, by_spot.at[0], cl_sem.at[1])
    kept_sums.start()
    sums_near = [
        small(by_plane, by_spot.at[e], planes + e, peer(plane, (spot + e) % inner)) for e in range(1, inner)
    ]

    near = []
    order = [(f, 0) for f in range(2)] + [(f, d) for f in range(2) for d in range(1, planes)]
    for f, d in order:
        g = f * planes + d
        if d == 0:
            far[g].wait()
        else:
            far[g].wait_recv()

        def place(t, carry, g=g):
            e = t // slots
            s = t % slots
            index = pos_ref[(spot + e) % inner, s]
            found = index < cap
            lines = held[g][jnp.where(found, index, 0)]
            stage[g][e, s] = jnp.where(found, lines, 0.0)
            return carry

        lax.fori_loop(0, inner * slots, place, 0)
        source = mate(d) * inner + spot
        for e in range(1, inner):
            copy = pltpu.make_async_remote_copy(
                src_ref=stage[g].at[e],
                dst_ref=outs[f].at[:, source],
                send_sem=is_sem.at[g * inner + e],
                recv_sem=ir_sem.at[g * inner + e],
                device_id=peer(plane, (spot + e) % inner),
                device_id_type=pl.DeviceIdType.MESH,
            )
            copy.start()
            near.append(copy)
        copy = pltpu.make_async_copy(stage[g].at[0], outs[f].at[:, source], self_sem.at[g])
        copy.start()
        near.append(copy)
    kept_sums.wait()
    for copy in sums_near:
        copy.wait()
    sums_across = [
        small(by_spot, by_group.at[g], planes + inner + g, (me, (core + g) % groups))
        for g in range(1, groups)
    ]
    oc_ref[core] = jnp.sum(by_spot[...], axis=(0, 1))
    for g in range(1, groups):
        sums_across[g - 1].wait()
        oc_ref[(core + groups - g) % groups] = jnp.sum(by_group[g], axis=(0, 1))
    for f in range(2):
        for d in range(1, planes):
            far[f * planes + d].wait_send()
    for copy in near:
        copy.wait()


def exchange(planes, inner, groups, slots, cap, branch, positions, sums, master_send, update_send):
    lines, lanes = master_send.shape[2:]
    shape = jax.ShapeDtypeStruct((slots, planes * inner, lines, lanes), jnp.float32)
    any_space = pl.BlockSpec(memory_space=pl.ANY)
    steps = 2 * planes
    tile = sums.shape
    hops = planes + inner + groups
    sent = (planes - 1) * cap * 2 * lines * lanes * 4
    return pl.pallas_call(
        functools.partial(exchange_kernel, planes, inner, groups, slots, cap),
        out_shape=(shape, shape, jax.ShapeDtypeStruct((groups, *tile), jnp.float32)),
        in_specs=[
            pl.BlockSpec(memory_space=pltpu.SMEM),
            pl.BlockSpec(memory_space=pltpu.VMEM),
            any_space,
            any_space,
        ],
        out_specs=(any_space, any_space, pl.BlockSpec(memory_space=pltpu.VMEM)),
        scratch_shapes=[pltpu.VMEM((cap, lines, lanes), jnp.float32)] * steps
        + [pltpu.VMEM((inner, slots, lines, lanes), jnp.float32)] * steps
        + [
            pltpu.SemaphoreType.DMA((steps,)),
            pltpu.SemaphoreType.DMA((steps,)),
            pltpu.SemaphoreType.DMA((2,)),
            pltpu.SemaphoreType.DMA((steps * inner,)),
            pltpu.SemaphoreType.DMA((steps * inner,)),
            pltpu.SemaphoreType.DMA((steps,)),
            pltpu.VMEM((planes, *tile), jnp.float32),
            pltpu.VMEM((inner, planes, *tile), jnp.float32),
            pltpu.VMEM((groups, inner, planes, *tile), jnp.float32),
            pltpu.SemaphoreType.DMA((hops,)),
            pltpu.SemaphoreType.DMA((hops,)),
            pltpu.SemaphoreType.DMA((2,)),
        ],
        cost_estimate=pl.CostEstimate(flops=0, bytes_accessed=sent * 4, transcendentals=0),
        compiler_params=pltpu.CompilerParams(
            collective_id=branch, has_side_effects=True, vmem_limit_bytes=60 * 1024 * 1024
        ),
    )(positions, sums, master_send, update_send)


def shards_general(number_base, single, master, first_moment, second_moment, rotation, assignment):
    dp_count = lax.axis_size("dp")
    group_count = lax.axis_size("expert")
    position = lax.axis_index("dp")
    round_count = rotation.shape[0]
    rows_here = master.shape[1]
    lane_count = LANE
    per_row = master.shape[2] // lane_count
    lines_device = rows_here * per_row
    piece_len = lines_device // (round_count * dp_count)
    inv_count = 1.0 / math.sqrt(dp_count * piece_len * lane_count)
    table = slot_table(rotation, dp_count, MOST)
    span_count = round_count * dp_count
    inner = INNER
    planes = dp_count // inner
    slots = round_count * MOST

    plane_of = rotation.reshape(span_count) // inner
    span_ids = jnp.arange(span_count, dtype=jnp.int32)
    same = (plane_of[:, None] == plane_of[None, :]) & (span_ids[None, :] < span_ids[:, None])
    place_of = jnp.sum(same.astype(jnp.int32), axis=1)
    plane_ids = jnp.arange(planes, dtype=jnp.int32)
    loads = jnp.sum((plane_of[None, :] == plane_ids[:, None]).astype(jnp.int32), axis=1)
    most_load = jnp.max(loads)
    cap_all = min(inner * slots, span_count)
    mean_load = span_count // planes
    shares = () if single else (10, 11, 12, 13, 14, 16)
    caps = sorted({min(cap_all, mean_load * eighths // 8) for eighths in shares} | {cap_all})
    choice = sum(((most_load > cap).astype(jnp.int32) for cap in caps[:-1]), jnp.int32(0))
    place_ids = jnp.arange(cap_all, dtype=jnp.int32)
    listed = (plane_of[None, None, :] == plane_ids[:, None, None]) & (
        place_of[None, None, :] == place_ids[None, :, None]
    )
    lists = jnp.sum(listed.astype(jnp.int32) * span_ids, axis=2)
    mine = table.transpose(2, 0, 1).reshape(planes, inner, round_count, MOST)
    mine = lax.dynamic_index_in_dim(mine, position // inner, 0, keepdims=False)
    padded_place = jnp.concatenate(
        [place_of.reshape(round_count, dp_count), jnp.full((round_count, 1), cap_all, jnp.int32)], axis=1
    )
    hits = mine[..., None] == jnp.arange(dp_count + 1, dtype=jnp.int32)
    positions = jnp.sum(hits * padded_place[None, :, None, :], axis=3).reshape(inner, slots)

    update = scaled_moment(first_moment, second_moment)
    master_lines = master.reshape(span_count, piece_len, lane_count)
    update_lines = update.reshape(span_count, piece_len, lane_count)
    local_lines = position * lines_device + jnp.arange(lines_device, dtype=jnp.int32).reshape(
        span_count, piece_len
    )
    weights = position_weights(local_lines, per_row, lane_count)
    master_sums = jnp.sum(master_lines * weights, axis=(1, 2)) * inv_count
    update_sums = jnp.sum(update_lines * weights, axis=(1, 2)) * inv_count

    permuting = (assignment[:, None] == span_ids[None, :]).astype(jnp.float32)
    both_sums = jnp.stack([master_sums, update_sums])
    placed_sums = jnp.sum(both_sums[:, :, None] * permuting[None], axis=1)
    entries = 2 * span_count
    tile_size = 8 * lane_count
    sums = jnp.pad(placed_sums.reshape(entries), (0, -entries % tile_size)).reshape(-1, lane_count)

    def branch_of(number, cap):
        def run(master_in, update_in):
            chosen = lists[:, :cap]
            return exchange(
                planes,
                inner,
                group_count,
                slots,
                cap,
                number_base + number,
                positions,
                sums,
                master_in[chosen],
                update_in[chosen],
            )

        return run

    saved_master, saved_update, totals = lax.switch(
        choice, [branch_of(number, cap) for number, cap in enumerate(caps)], master_lines, update_lines
    )
    checksums = totals.reshape(group_count, -1)[:, :entries].reshape(group_count, 2, span_count)
    shape_out = (1, round_count, MOST, dp_count * piece_len, lane_count)
    return (saved_master.reshape(shape_out), saved_update.reshape(shape_out), checksums)


LIST = 2
SELF = LIST + 6
NEAR = SELF + 3
DIAG = NEAR + 2
TABLES = DIAG + 1


def table_kernel(books, most_slots, rot_ref, tab_ref, choice_ref):
    rounds, _, dp_count = rot_ref.shape
    spans = rounds * dp_count
    me = lax.axis_index("dp")
    z, y, x = me // 4, (me // 2) % 2, me % 2
    mate = z + 1 - 2 * (z % 2)
    lane = lax.broadcasted_iota(jnp.int32, (1, LANE), 1)
    sub = lax.broadcasted_iota(jnp.int32, (8, LANE), 0)
    row = jnp.full((1, LANE), -1, jnp.int32)
    blocks = []
    for c in range(spans):
        if c % 8 == 0:
            block = jnp.zeros((8, LANE), jnp.int32)
        w = rot_ref[c // dp_count, 0, c % dp_count]
        row = jnp.where(lane == c, w, row)
        block = jnp.where(sub == c % 8, w, block)
        if c % 8 == 7:
            blocks.append(block)
    shape = (spans, LANE)
    writer = jnp.concatenate(blocks, axis=0)
    writer_across = jnp.broadcast_to(row, shape)
    span = lax.broadcasted_iota(jnp.int32, shape, 0)
    across = lax.broadcasted_iota(jnp.int32, shape, 1)
    before = across < span

    def rank(same):
        return jnp.sum(jnp.where(same & before, 1.0, 0.0), axis=1, keepdims=True)

    def spread(values):
        return jnp.broadcast_to(values.astype(jnp.int32), shape)

    def plane_of(w):
        return lax.shift_right_arithmetic(w, 2)

    def bit(w, n):
        return lax.shift_right_arithmetic(w, n) & 1

    plane, plane_across = plane_of(writer), plane_of(writer_across)
    same_plane = plane == plane_across
    in_plane_f = rank(same_plane)
    half_f = rank(lax.shift_right_arithmetic(writer, 3) == lax.shift_right_arithmetic(writer_across, 3))
    round_of, round_across = span // dp_count, across // dp_count
    turn = spread(rank((writer == writer_across) & (round_of == round_across)))
    outer = [jnp.sum(jnp.where(plane == p, 1, 0), axis=0, keepdims=True) for p in (0, 3)]
    in_plane = spread(in_plane_f)
    in_half = in_plane + jnp.where(plane == 1, outer[0], 0) + jnp.where(plane == 2, outer[1], 0)
    slot = round_of * most_slots + turn
    share = rounds * most_slots // 2

    def held_by(other):
        return jnp.sum(jnp.where((writer ^ other) == writer_across, 1.0, 0.0), axis=1, keepdims=True).astype(jnp.int32)

    count = [held_by(other) for other in range(4)]

    def along_x(near_x, near_y, diagonal):
        even = lax.shift_right_arithmetic(near_y + diagonal - near_x, 1)
        return jnp.minimum(jnp.maximum(even, jnp.maximum(diagonal - share, 0)), jnp.minimum(diagonal, share))

    order = rank(writer == writer_across).astype(jnp.int32)
    split = along_x(count[2], count[1], count[0])
    near = [
        order + along_x(count[0], count[3], count[2]),
        order + count[1] - along_x(count[3], count[0], count[1]),
    ]
    longest = [jnp.max((n - order + count[0]).astype(jnp.float32)) for n in near]
    by_x = order < split
    far = [jnp.where(by_x, order, LANE), jnp.where(by_x, LANE, order - split)]
    joint = jnp.where(by_x, order, share + order - split)

    def put(number, mask, value, absent):
        picked = jnp.sum(jnp.where(mask, value - absent, 0), axis=0, keepdims=True)
        tab_ref[pl.ds(number, 1), :] = picked + absent

    put(0, (lax.shift_right_arithmetic(writer, 3) != z // 2) & (in_half == across), span, 0)
    put(1, (plane == mate) & (in_plane == across), span, 0)
    for a in range(2):
        to_near, to_far = writer == (me ^ (1 + a)), writer == (me ^ 3)
        mask = (to_near & (spread(near[a]) == across)) | (to_far & (spread(far[a]) == across))
        for kind, value in enumerate((span, in_plane, in_half)):
            put(LIST + a * 3 + kind, mask, value, 0)
    at_slot = (writer == me) & (slot == across)
    places = (span, in_plane, in_half, spread(near[0]), spread(near[1]), spread(joint))
    for number, value in enumerate(places):
        put(SELF + number, at_slot, value, -1)
    most_half, most_plane = jnp.max(half_f) + 1.0, jnp.max(in_plane_f) + 1.0
    most_col = jnp.maximum(longest[0], longest[1])
    choice = jnp.int32(len(books))
    for number in reversed(range(len(books))):
        cap_half, cap_plane, cap_col = books[number]
        fits = (most_half <= cap_half) & (most_plane <= cap_plane) & (most_col <= cap_col)
        choice = jnp.where(fits, number, choice)
    choice_ref[0] = choice


def tables_of(rotation, books):
    smem = pl.BlockSpec(memory_space=pltpu.SMEM)
    return pl.pallas_call(
        functools.partial(table_kernel, books, MOST),
        out_shape=(jax.ShapeDtypeStruct((TABLES, LANE), jnp.int32), jax.ShapeDtypeStruct((1,), jnp.int32)),
        in_specs=[smem],
        out_specs=(pl.BlockSpec(memory_space=pltpu.VMEM), smem),
    )(rotation.transpose(0, 2, 1))


def deliver_kernel(saved_ref, totals_ref, om_ref, ou_ref, oc_ref, held, in_sem, out_sem):
    slots = om_ref.shape[0]
    takes = []
    for f in range(2):
        for q in range(slots):
            n = f * slots + q
            takes.append(pltpu.make_async_copy(saved_ref.at[f, q], held.at[n], in_sem.at[n]))
            takes[n].start()
    oc_ref[...] = totals_ref[:, : oc_ref.shape[1], : oc_ref.shape[2]]
    gives = []
    for f, out_ref in enumerate((om_ref, ou_ref)):
        for q in range(slots):
            n = f * slots + q
            takes[n].wait()
            gives.append(pltpu.make_async_copy(held.at[n], out_ref.at[q], out_sem.at[n]))
            gives[n].start()
    for give in gives:
        give.wait()


def deliver(saved, totals, spans):
    slots = saved.shape[1]
    any_space = pl.BlockSpec(memory_space=pl.ANY)
    vmem = pl.BlockSpec(memory_space=pltpu.VMEM)
    out = jax.ShapeDtypeStruct(saved.shape[1:], jnp.float32)
    return pl.pallas_call(
        deliver_kernel,
        out_shape=(out, out, jax.ShapeDtypeStruct((totals.shape[0], 2, spans), jnp.float32)),
        in_specs=[any_space, vmem],
        out_specs=(any_space, any_space, vmem),
        scratch_shapes=[
            pltpu.VMEM((2 * slots, *saved.shape[2:]), jnp.float32),
            pltpu.SemaphoreType.DMA((2 * slots,)),
            pltpu.SemaphoreType.DMA((2 * slots,)),
        ],
        cost_estimate=pl.CostEstimate(flops=0, bytes_accessed=saved.size * 8, transcendentals=0),
        compiler_params=pltpu.CompilerParams(vmem_limit_bytes=48 * 1024 * 1024),
    )(saved, totals)


def fast_kernel(
    spans, slots, parts, lines, groups, inv_count, cap_half, cap_plane, cap_col,
    tab, asg_ref, wt_ref, m_ref, a_ref, b_ref, out_ref, oc_ref,
    raw_m, raw_a, raw_b, fld, xs, zs, lz, lc, fs, lf, lg, ss, work, rows_ref, sums, sums_in, across,
    load_sem, xs_sem, lc_sem, zs_sem, lz_sem, fw_sem, fs_sem, lf_sem, gs_sem, lg_sem, ss_sem, cs_sem, cr_sem,
):
    steps = 2 * parts
    ring = fs.shape[1]
    share = slots // 2
    me = lax.axis_index("dp")
    core = lax.axis_index("expert")
    z, y, x = me // 4, (me // 2) % 2, me % 2
    spot = me % 4
    inner = (z == 1) | (z == 2)
    outer = (z == 0) | (z == 3)
    outer_int = ((z + 1) // 2 + 1) % 2
    mate_x = me + 1 - 2 * x
    mate_y = me + 2 - 4 * y
    z_one = z + 1 - 2 * (z % 2)
    z_two = z + 2 - 4 * (z // 2)
    z_three = 3 - z
    mate_z = z_one * 4 + spot
    cross_to = (2 - z // 2) * 4 + spot
    plane_of = (
        z,
        z_one,
        z_two + outer_int * (z_three - z_two),
        z_three + outer_int * (z_two - z_three),
    )

    def to(dp_index):
        return (dp_index, core)

    def remote(src, dst, send, recv, target):
        return pltpu.make_async_remote_copy(
            src_ref=src,
            dst_ref=dst,
            send_sem=send,
            recv_sem=recv,
            device_id=target,
            device_id_type=pl.DeviceIdType.MESH,
        )

    loads = [
        pltpu.make_async_copy(ref, raw, load_sem.at[n])
        for n, (ref, raw) in enumerate(((m_ref, raw_m), (a_ref, raw_a), (b_ref, raw_b)))
    ]
    loads[0].start()
    barrier = pltpu.get_barrier_semaphore()
    for target in (mate_x, mate_y, mate_z, z_two * 4 + spot, z_three * 4 + spot):
        pl.semaphore_signal(barrier, inc=1, device_id=to(target), device_id_type=pl.DeviceIdType.MESH)
    for g in range(1, groups):
        pl.semaphore_signal(
            barrier, inc=1, device_id=(me, (core + g) % groups), device_id_type=pl.DeviceIdType.MESH
        )
    pl.semaphore_wait(barrier, 4 + groups)

    def relay(raw, k):
        i = k % parts

        def step(c, carry):
            row = c * parts + i
            start = (row // 8) * (8 * lines) + row % 8
            fld[k, c] = raw[pl.ds(start, lines, stride=8), :]
            return carry

        lax.fori_loop(0, spans, step, 0)

    def pick(count, row, load, store):
        def step(t, carry):
            for u in range(2):
                store(2 * t + u, load(tab[row, 2 * t + u]))
            return carry

        lax.fori_loop(0, count // 2, step, 0)
        if count % 2:
            store(count - 1, load(tab[row, count - 1]))

    def load_from(j, k):
        if j == 0:
            return lambda n: fld[k, n]
        return lambda n: work[n]

    def take(count, offset, ref, *at):
        def step(t, carry):
            for u in range(2):
                work[offset + 2 * t + u] = ref[(*at, 2 * t + u)]
            return carry

        lax.fori_loop(0, count // 2, step, 0)
        if count % 2:
            work[offset + count - 1] = ref[(*at, count - 1)]

    def cross_copy(k):
        return remote(
            xs.at[k], lc.at[1 - outer_int, k], xs_sem.at[k], lc_sem.at[1 - outer_int, k], to(cross_to)
        )

    def plane_copy(k):
        return remote(zs.at[k], lz.at[k], zs_sem.at[k], lz_sem.at[k], to(mate_z))

    def forward_copy(s, k):
        return remote(
            lc.at[s, k, pl.ds(0, cap_plane)],
            lc.at[s, k, pl.ds(0, cap_plane)],
            fw_sem.at[s, k],
            lc_sem.at[s, k],
            to(mate_z),
        )

    mates = (mate_x, mate_y)
    spots = (spot, mate_x % 4, mate_y % 4, 3 - spot)

    def first_copy(a, j, k):
        r = k % ring
        return remote(fs.at[a, r, j], lf.at[a, k, j], fs_sem.at[a, r, j], lf_sem.at[a, k, j], to(mates[a]))

    def onward_copy(a, j, k):
        return remote(
            lf.at[a, k, j, pl.ds(0, share)], lg.at[a, k, j], gs_sem.at[a, k, j], lg_sem.at[a, k, j], to(mates[1 - a])
        )

    def out_copy(j, where, k):
        n = j * 4 + where
        place = out_ref.at[k // parts, :, plane_of[j] * 4 + spots[where], pl.ds((k % parts) * lines, lines)]
        return pltpu.make_async_copy(ss.at[n, k % 2], place, ss_sem.at[n, k % 2])

    def place_out(j, where, k, row, load):
        copy = out_copy(j, where, k)

        @pl.when(k >= 2)
        def _():
            copy.wait()

        for q in range(slots):
            index = tab[row, q]
            found = index >= 0
            value = load(jnp.where(found, index, 0))
            ss[j * 4 + where, k % 2, q] = jnp.where(found, value, 0.0)
        copy.start()

    def both_hops(j, k):
        kind = min(j, 2)
        for a in range(2):
            copy = first_copy(a, j, k)

            @pl.when(k >= ring)
            def _(copy=copy):
                copy.wait_send()

            def store(t, value, a=a):
                fs[a, k % ring, j, t] = value

            pick(cap_col, LIST + a * 3 + kind, load_from(j, k), store)
            copy.start()
        place_out(j, 0, k, SELF + kind, load_from(j, k))

    def near_list(j, k):
        for a in range(2):
            first_copy(a, j, k).wait_recv()
            onward_copy(a, j, k).start()
            take(cap_col, 0, lf, a, k, j)
            place_out(j, 1 + a, k, NEAR + a, load_from(1, k))

    def diag_list(j, k):
        for a in range(2):
            onward_copy(a, j, k).wait_recv()
            take(share, a * share, lg, a, k, j)
        place_out(j, 3, k, DIAG, load_from(1, k))

    def late(run, j, k, lag):
        @pl.when((k >= lag) & (k < steps + lag))
        def _():
            run(j, k - lag)

    def own_list(raw):
        def step(k, carry):
            relay(raw, k)

            def store_x(t, value):
                xs[k, t] = value

            def store_z(t, value):
                zs[k, t] = value

            pick(cap_half, 0, load_from(0, k), store_x)
            cross_copy(k).start()

            @pl.when(inner)
            def _():
                pick(cap_plane, 1, load_from(0, k), store_z)
                plane_copy(k).start()

            both_hops(0, k)
            return carry

        return step

    loads[0].wait()
    loads[1].start()
    loads[2].start()
    lax.fori_loop(0, parts, own_list(raw_m), 0)
    loads[1].wait()
    loads[2].wait()
    corr_one = 1.0 - BETA_ONE**STEP
    corr_two = 1.0 - BETA_TWO**STEP

    def moments(t, carry):
        at = pl.ds(t * 64, 64)
        raw_a[at, :] = raw_a[at, :] * (1.0 / corr_one) / (jnp.sqrt(raw_b[at, :] * (1.0 / corr_two)) + EPSILON)
        return carry

    lax.fori_loop(0, raw_a.shape[0] // 64, moments, 0)
    lax.fori_loop(parts, steps, own_list(raw_a), 0)

    @pl.when(outer)
    def _():
        def step(k, carry):
            def store_z(t, value):
                zs[k, t] = value

            pick(cap_plane, 1, load_from(0, k), store_z)
            plane_copy(k).start()
            return carry

        lax.fori_loop(0, steps, step, 0)

    sums[0] = jnp.zeros(sums.shape[1:], jnp.float32)
    for f in range(2):
        def one_piece(c, carry, f=f):
            total = jnp.zeros(fld.shape[2:], jnp.float32)
            for i in range(parts):
                row = (me * spans + c) * parts + i
                total = total + fld[f * parts + i, c] * wt_ref[(row * 5) % 11]
            rows_ref[pl.ds(c, 1), :] = jnp.sum(total, axis=0, keepdims=True)
            return carry

        lax.fori_loop(0, spans, one_piece, 0)
        per_span = jnp.sum(rows_ref[...], axis=1, keepdims=True) * inv_count
        rows_ref[...] = jnp.broadcast_to(per_span, rows_ref.shape)
        slot_of = lax.broadcasted_iota(jnp.int32, (1, rows_ref.shape[1]), 1)

        def one_place(c, placed):
            return placed + jnp.where(slot_of == asg_ref[c], rows_ref[pl.ds(c, 1), :], 0.0)

        sums[0, pl.ds(f, 1), :] = lax.fori_loop(0, spans, one_place, jnp.zeros(slot_of.shape, jnp.float32))

    turns = (mate_x, mate_y, mate_z, z_two * 4 + spot)

    def turn_copy(t):
        return remote(sums.at[t], sums_in.at[t], cs_sem.at[t], cr_sem.at[t], to(turns[t]))

    def turn_end(t):
        turn_copy(t).wait()
        sums[t + 1] = sums[t] + sums_in[t]

    turn_copy(0).start()

    def sums_at(k, base):
        for t in range(3):
            @pl.when(k == base + 3 * t)
            def _(t=t):
                turn_end(t)
                turn_copy(t + 1).start()

    def plane_list(j, k):
        plane_copy(k).wait_recv()
        take(cap_plane, 0, lz, k)
        both_hops(1, k)

    @pl.when(inner)
    def _():
        def crossed(j, k):
            s = j - 2
            remote(xs.at[k], lc.at[s, k], xs_sem.at[k], lc_sem.at[s, k], to(cross_to)).wait_recv()
            forward_copy(s, k).start()
            take(cap_half, 0, lc, s, k)
            both_hops(j, k)

        def step(k, carry):
            late(near_list, 0, k, 0)
            late(crossed, 2, k, 0)
            late(near_list, 2, k, 1)
            late(diag_list, 0, k, 1)
            late(diag_list, 2, k, 2)
            return carry

        lax.fori_loop(0, steps + 2, step, 0)

        def step_far(k, carry):
            late(plane_list, 1, k, 0)
            late(crossed, 3, k, 0)
            late(near_list, 1, k, 1)
            late(near_list, 3, k, 1)
            late(diag_list, 1, k, 2)
            late(diag_list, 3, k, 2)
            sums_at(k, 1)
            return carry

        lax.fori_loop(0, steps + 2, step_far, 0)

        def drain(k, carry):
            for s in range(2):
                forward_copy(s, k).wait_send()
            return carry

        lax.fori_loop(0, steps, drain, 0)

    @pl.when(outer)
    def _():
        def forwarded(j, k):
            s = j - 2
            forward_copy(s, k).wait_recv()
            take(cap_plane, 0, lc, s, k)
            both_hops(j, k)

        def step_near(k, carry):
            late(plane_list, 1, k, 0)
            late(near_list, 0, k, 0)
            late(diag_list, 0, k, 1)
            return carry

        lax.fori_loop(0, steps + 1, step_near, 0)

        def step(k, carry):
            late(forwarded, 2, k, 0)
            late(near_list, 1, k, 0)
            late(near_list, 2, k, 1)
            late(diag_list, 1, k, 1)
            late(diag_list, 2, k, 2)
            return carry

        lax.fori_loop(0, steps + 2, step, 0)

        def step_far(k, carry):
            late(forwarded, 3, k, 0)
            late(near_list, 3, k, 1)
            late(diag_list, 3, k, 2)
            sums_at(k, 1)
            return carry

        lax.fori_loop(0, steps + 2, step_far, 0)

    turn_end(3)
    sent_across = []
    for g in range(1, groups):
        copy = remote(sums.at[4], across.at[g], cs_sem.at[3 + g], cr_sem.at[3 + g], (me, (core + g) % groups))
        copy.start()
        sent_across.append(copy)

    def finish(k, carry):
        cross_copy(k).wait_send()
        plane_copy(k).wait_send()
        for j in range(4):
            for a in range(2):
                onward_copy(a, j, k).wait_send()
        return carry

    lax.fori_loop(0, steps, finish, 0)

    def finish_ring(k, carry):
        for j in range(4):
            for a in range(2):
                first_copy(a, j, k).wait_send()
        return carry

    lax.fori_loop(steps - ring, steps, finish_ring, 0)

    def finish_own(k, carry):
        for j in range(4):
            for where in range(4):
                out_copy(j, where, k).wait()
        return carry

    lax.fori_loop(steps - 2, steps, finish_own, 0)
    oc_ref[core] = sums[4]
    for g in range(1, groups):
        sent_across[g - 1].wait()
        oc_ref[(core + groups - g) % groups] = across[g]


def fast_exchange(number, book, slots, spans, parts, lines, lanes, groups, inv_count, tab, places, weights, m_in, a_in, b_in):
    cap_half, cap_plane, cap_col = book
    steps = 2 * parts
    ring = (parts + 1) // 2
    dp_count = lax.axis_size("dp")
    share = slots // 2
    any_space = pl.BlockSpec(memory_space=pl.ANY)
    vmem = pl.BlockSpec(memory_space=pltpu.VMEM)
    smem = pl.BlockSpec(memory_space=pltpu.SMEM)

    def pieces(*lead):
        return pltpu.VMEM((*lead, lines, lanes), jnp.float32)

    def sems(*lead):
        return pltpu.SemaphoreType.DMA(lead)

    raw = pltpu.VMEM(m_in.shape, jnp.float32)
    return pl.pallas_call(
        functools.partial(fast_kernel, spans, slots, parts, lines, groups, inv_count, cap_half, cap_plane, cap_col),
        out_shape=(
            jax.ShapeDtypeStruct((2, slots, dp_count, parts * lines, lanes), jnp.float32),
            jax.ShapeDtypeStruct((groups, 8, lanes), jnp.float32),
        ),
        in_specs=[smem, smem, vmem, any_space, any_space, any_space],
        out_specs=(any_space, vmem),
        scratch_shapes=[
            raw,
            raw,
            raw,
            pieces(steps, spans),
            pieces(steps, cap_half),
            pieces(steps, cap_plane),
            pieces(steps, cap_plane),
            pieces(2, steps, cap_half),
            pieces(2, ring, 4, cap_col),
            pieces(2, steps, 4, cap_col),
            pieces(2, steps, 4, share),
            pieces(16, 2, slots),
            pieces(cap_half),
            pltpu.VMEM((spans, lanes), jnp.float32),
            pltpu.VMEM((5, 8, lanes), jnp.float32),
            pltpu.VMEM((4, 8, lanes), jnp.float32),
            pltpu.VMEM((groups, 8, lanes), jnp.float32),
            sems(3),
            sems(steps),
            sems(2, steps),
            sems(steps),
            sems(steps),
            sems(2, steps),
            sems(2, ring, 4),
            sems(2, steps, 4),
            sems(2, steps, 4),
            sems(2, steps, 4),
            sems(16, 2),
            sems(3 + groups),
            sems(3 + groups),
        ],
        cost_estimate=pl.CostEstimate(flops=0, bytes_accessed=4 * m_in.size * 8, transcendentals=0),
        compiler_params=pltpu.CompilerParams(
            collective_id=number, has_side_effects=True, vmem_limit_bytes=67043328
        ),
    )(tab, places, weights, m_in, a_in, b_in)


def shards(master, first_moment, second_moment, rotation, assignment):
    dp_count = lax.axis_size("dp")
    group_count = lax.axis_size("expert")
    round_count = rotation.shape[0]
    rows_here, columns = master.shape[1:]
    lines = columns // LANE
    span_count = round_count * dp_count
    slots = round_count * MOST
    parts = rows_here // span_count
    if dp_count != INNER * 4 or 8 * lines * (rows_here // 8) * LANE != rows_here * columns or span_count > LANE:
        return shards_general(0, False, master, first_moment, second_moment, rotation, assignment)

    half = span_count // 2
    books = (
        (half * 9 // 8, half * 3 // 4, slots),
        (half * 19 // 16, half * 25 // 32, slots + 1),
        (half * 5 // 4, half * 13 // 16, slots + 2),
        (half * 43 // 32, half * 7 // 8, slots + 3),
    )
    inv_count = 1.0 / math.sqrt(dp_count * parts * lines * LANE)
    tab, choice = tables_of(rotation, books)
    places = assignment
    pattern = np.arange(11)[:, None] + 3 * np.arange(columns)[None, :]
    weights = (1.0 + (pattern % 11).astype(np.float32) / np.float32(10.0)).astype(np.float32)
    weights = jnp.asarray(weights.reshape(11, lines, LANE))

    def tile_order(array):
        return array.reshape(rows_here // 8, 8, lines, LANE).transpose(0, 2, 1, 3).reshape(rows_here * lines, LANE)

    def fast(number, book):
        def run(tab_in, master_in, first_in, second_in):
            return fast_exchange(
                number, book, slots, span_count, parts, lines, LANE, group_count, inv_count,
                tab_in, places, weights, tile_order(master_in), tile_order(first_in), tile_order(second_in),
            )

        return run

    def general(tab_in, master_in, first_in, second_in):
        kept = shards_general(len(books), True, master_in, first_in, second_in, rotation, assignment)
        both = [saved.reshape(slots, dp_count, parts * lines, LANE) for saved in kept[:2]]
        return jnp.stack(both), jnp.pad(kept[2], ((0, 0), (0, 6), (0, LANE - span_count)))

    branches = [fast(number, book) for number, book in enumerate(books)] + [general]
    saved, totals = lax.switch(choice[0], branches, tab, master, first_moment, second_moment)
    saved_master, saved_update, checksums = deliver(saved, totals, span_count)
    shape_out = (1, round_count, MOST, dp_count * parts * lines, LANE)
    return saved_master.reshape(shape_out), saved_update.reshape(shape_out), checksums


def solution(mesh):
    placed = (P("expert", "dp", None), P("expert", "dp", None), P("expert", "dp", None), P(), P())
    return jax.shard_map(
        shards,
        mesh=mesh,
        in_specs=placed,
        out_specs=(P("expert", "dp", None, None, None), P("expert", "dp", None, None, None), P()),
        check_vma=False,
    )
```

```python
import functools
import math

import jax
import jax.numpy as jnp
import numpy as np
from jax import lax
from jax.experimental import pallas as pl
from jax.experimental.pallas import tpu as pltpu
from jax.sharding import PartitionSpec as P

LANE = 128
MOST = 3
STEP = 20
INNER = 4


BETA_ONE = 0.9
BETA_TWO = 0.95
EPSILON = 1e-08


def scaled_moment(first_part, second_part):
    corr_one = 1.0 - BETA_ONE**STEP
    corr_two = 1.0 - BETA_TWO**STEP
    return first_part / corr_one / (jnp.sqrt(second_part / corr_two) + EPSILON)


def slot_table(rotation, dp_count, most_slots):
    owners = rotation[:, :, 0]
    span_ids = jnp.arange(dp_count, dtype=jnp.int32)
    same_writer = owners[:, :, None] == owners[:, None, :]
    before = span_ids[None, :] < span_ids[:, None]
    slot_rank = jnp.sum((same_writer & before[None]).astype(jnp.int32), axis=2)
    writers = jnp.arange(dp_count, dtype=jnp.int32)
    slot_ids = jnp.arange(most_slots, dtype=jnp.int32)
    matches = (owners[:, None, None, :] == writers[None, None, :, None]) & (
        slot_rank[:, None, None, :] == slot_ids[None, :, None, None]
    )
    matches = matches.astype(jnp.int32)
    found_any = jnp.sum(matches, axis=3)
    picked = jnp.sum(matches * span_ids, axis=3)
    return picked + (1 - found_any) * dp_count


def position_weights(line_ids, per_row, lane_count):
    row_ids = line_ids // per_row
    col_ids = line_ids % per_row * lane_count
    lane_ids = jnp.arange(lane_count, dtype=jnp.int32)
    pattern = (row_ids[..., None] * 5 + (col_ids[..., None] + lane_ids) * 3) % 11
    return 1.0 + pattern.astype(jnp.float32) / 10.0


def exchange_kernel(
    planes, inner, groups, slots, cap, pos_ref, sum_ref, m_ref, u_ref, om_ref, ou_ref, oc_ref, *scratch
):
    held = scratch[: 2 * planes]
    stage = scratch[2 * planes : 4 * planes]
    zs_sem, zr_sem, local_sem, is_sem, ir_sem, self_sem = scratch[4 * planes : 4 * planes + 6]
    by_plane, by_spot, by_group, cs_sem, cr_sem, cl_sem = scratch[4 * planes + 6 :]
    me = lax.axis_index("dp")
    plane = me // inner
    spot = me % inner
    core = lax.axis_index("expert")
    fields = (m_ref, u_ref)
    outs = (om_ref, ou_ref)

    def peer(plane_to, spot_to):
        return (plane_to * inner + spot_to, core)

    def mate(d):
        other, bit = plane, 1
        while bit < planes:
            if d & bit:
                other = other + bit * (1 - 2 * ((plane // bit) % 2))
            bit *= 2
        return other

    barrier = pltpu.get_barrier_semaphore()
    for d in range(1, planes):
        pl.semaphore_signal(
            barrier, inc=1, device_id=peer(mate(d), spot), device_id_type=pl.DeviceIdType.MESH
        )
    for e in range(1, inner):
        pl.semaphore_signal(
            barrier, inc=1, device_id=peer(plane, (spot + e) % inner), device_id_type=pl.DeviceIdType.MESH
        )
    for g in range(1, groups):
        pl.semaphore_signal(
            barrier, inc=1, device_id=(me, (core + g) % groups), device_id_type=pl.DeviceIdType.MESH
        )
    pl.semaphore_wait(barrier, planes + inner + groups - 3)

    def small(src, dst, number, to):
        copy = pltpu.make_async_remote_copy(
            src_ref=src,
            dst_ref=dst,
            send_sem=cs_sem.at[number],
            recv_sem=cr_sem.at[number],
            device_id=to,
            device_id_type=pl.DeviceIdType.MESH,
        )
        copy.start()
        return copy

    own_sums = pltpu.make_async_copy(sum_ref, by_plane.at[0], cl_sem.at[0])
    own_sums.start()
    sums_far = [
        small(sum_ref, by_plane.at[d], d, peer(mate(d), spot)) for d in range(1, planes)
    ]

    far = [None] * (2 * planes)
    for f in range(2):
        own = pltpu.make_async_copy(fields[f].at[plane], held[f * planes], local_sem.at[f])
        own.start()
        far[f * planes] = own
        for d in range(1, planes):
            to_plane = mate(d)
            copy = pltpu.make_async_remote_copy(
                src_ref=fields[f].at[to_plane],
                dst_ref=held[f * planes + d],
                send_sem=zs_sem.at[f * planes + d],
                recv_sem=zr_sem.at[f * planes + d],
                device_id=peer(to_plane, spot),
                device_id_type=pl.DeviceIdType.MESH,
            )
            copy.start()
            far[f * planes + d] = copy

    own_sums.wait()
    for copy in sums_far:
        copy.wait()
    kept_sums = pltpu.make_async_copy(by_plane, by_spot.at[0], cl_sem.at[1])
    kept_sums.start()
    sums_near = [
        small(by_plane, by_spot.at[e], planes + e, peer(plane, (spot + e) % inner)) for e in range(1, inner)
    ]

    near = []
    order = [(f, 0) for f in range(2)] + [(f, d) for f in range(2) for d in range(1, planes)]
    for f, d in order:
        g = f * planes + d
        if d == 0:
            far[g].wait()
        else:
            far[g].wait_recv()

        def place(t, carry, g=g):
            e = t // slots
            s = t % slots
            index = pos_ref[(spot + e) % inner, s]
            found = index < cap
            lines = held[g][jnp.where(found, index, 0)]
            stage[g][e, s] = jnp.where(found, lines, 0.0)
            return carry

        lax.fori_loop(0, inner * slots, place, 0)
        source = mate(d) * inner + spot
        for e in range(1, inner):
            copy = pltpu.make_async_remote_copy(
                src_ref=stage[g].at[e],
                dst_ref=outs[f].at[:, source],
                send_sem=is_sem.at[g * inner + e],
                recv_sem=ir_sem.at[g * inner + e],
                device_id=peer(plane, (spot + e) % inner),
                device_id_type=pl.DeviceIdType.MESH,
            )
            copy.start()
            near.append(copy)
        copy = pltpu.make_async_copy(stage[g].at[0], outs[f].at[:, source], self_sem.at[g])
        copy.start()
        near.append(copy)
    kept_sums.wait()
    for copy in sums_near:
        copy.wait()
    sums_across = [
        small(by_spot, by_group.at[g], planes + inner + g, (me, (core + g) % groups))
        for g in range(1, groups)
    ]
    oc_ref[core] = jnp.sum(by_spot[...], axis=(0, 1))
    for g in range(1, groups):
        sums_across[g - 1].wait()
        oc_ref[(core + groups - g) % groups] = jnp.sum(by_group[g], axis=(0, 1))
    for f in range(2):
        for d in range(1, planes):
            far[f * planes + d].wait_send()
    for copy in near:
        copy.wait()


def exchange(planes, inner, groups, slots, cap, branch, positions, sums, master_send, update_send):
    lines, lanes = master_send.shape[2:]
    shape = jax.ShapeDtypeStruct((slots, planes * inner, lines, lanes), jnp.float32)
    any_space = pl.BlockSpec(memory_space=pl.ANY)
    steps = 2 * planes
    tile = sums.shape
    hops = planes + inner + groups
    sent = (planes - 1) * cap * 2 * lines * lanes * 4
    return pl.pallas_call(
        functools.partial(exchange_kernel, planes, inner, groups, slots, cap),
        out_shape=(shape, shape, jax.ShapeDtypeStruct((groups, *tile), jnp.float32)),
        in_specs=[
            pl.BlockSpec(memory_space=pltpu.SMEM),
            pl.BlockSpec(memory_space=pltpu.VMEM),
            any_space,
            any_space,
        ],
        out_specs=(any_space, any_space, pl.BlockSpec(memory_space=pltpu.VMEM)),
        scratch_shapes=[pltpu.VMEM((cap, lines, lanes), jnp.float32)] * steps
        + [pltpu.VMEM((inner, slots, lines, lanes), jnp.float32)] * steps
        + [
            pltpu.SemaphoreType.DMA((steps,)),
            pltpu.SemaphoreType.DMA((steps,)),
            pltpu.SemaphoreType.DMA((2,)),
            pltpu.SemaphoreType.DMA((steps * inner,)),
            pltpu.SemaphoreType.DMA((steps * inner,)),
            pltpu.SemaphoreType.DMA((steps,)),
            pltpu.VMEM((planes, *tile), jnp.float32),
            pltpu.VMEM((inner, planes, *tile), jnp.float32),
            pltpu.VMEM((groups, inner, planes, *tile), jnp.float32),
            pltpu.SemaphoreType.DMA((hops,)),
            pltpu.SemaphoreType.DMA((hops,)),
            pltpu.SemaphoreType.DMA((2,)),
        ],
        cost_estimate=pl.CostEstimate(flops=0, bytes_accessed=sent * 4, transcendentals=0),
        compiler_params=pltpu.CompilerParams(
            collective_id=branch, has_side_effects=True, vmem_limit_bytes=60 * 1024 * 1024
        ),
    )(positions, sums, master_send, update_send)


def shards_general(number_base, single, master, first_moment, second_moment, rotation, assignment):
    dp_count = lax.axis_size("dp")
    group_count = lax.axis_size("expert")
    position = lax.axis_index("dp")
    round_count = rotation.shape[0]
    rows_here = master.shape[1]
    lane_count = LANE
    per_row = master.shape[2] // lane_count
    lines_device = rows_here * per_row
    piece_len = lines_device // (round_count * dp_count)
    inv_count = 1.0 / math.sqrt(dp_count * piece_len * lane_count)
    table = slot_table(rotation, dp_count, MOST)
    span_count = round_count * dp_count
    inner = INNER
    planes = dp_count // inner
    slots = round_count * MOST

    plane_of = rotation.reshape(span_count) // inner
    span_ids = jnp.arange(span_count, dtype=jnp.int32)
    same = (plane_of[:, None] == plane_of[None, :]) & (span_ids[None, :] < span_ids[:, None])
    place_of = jnp.sum(same.astype(jnp.int32), axis=1)
    plane_ids = jnp.arange(planes, dtype=jnp.int32)
    loads = jnp.sum((plane_of[None, :] == plane_ids[:, None]).astype(jnp.int32), axis=1)
    most_load = jnp.max(loads)
    cap_all = min(inner * slots, span_count)
    mean_load = span_count // planes
    shares = () if single else (10, 11, 12, 13, 14, 16)
    caps = sorted({min(cap_all, mean_load * eighths // 8) for eighths in shares} | {cap_all})
    choice = sum(((most_load > cap).astype(jnp.int32) for cap in caps[:-1]), jnp.int32(0))
    place_ids = jnp.arange(cap_all, dtype=jnp.int32)
    listed = (plane_of[None, None, :] == plane_ids[:, None, None]) & (
        place_of[None, None, :] == place_ids[None, :, None]
    )
    lists = jnp.sum(listed.astype(jnp.int32) * span_ids, axis=2)
    mine = table.transpose(2, 0, 1).reshape(planes, inner, round_count, MOST)
    mine = lax.dynamic_index_in_dim(mine, position // inner, 0, keepdims=False)
    padded_place = jnp.concatenate(
        [place_of.reshape(round_count, dp_count), jnp.full((round_count, 1), cap_all, jnp.int32)], axis=1
    )
    hits = mine[..., None] == jnp.arange(dp_count + 1, dtype=jnp.int32)
    positions = jnp.sum(hits * padded_place[None, :, None, :], axis=3).reshape(inner, slots)

    update = scaled_moment(first_moment, second_moment)
    master_lines = master.reshape(span_count, piece_len, lane_count)
    update_lines = update.reshape(span_count, piece_len, lane_count)
    local_lines = position * lines_device + jnp.arange(lines_device, dtype=jnp.int32).reshape(
        span_count, piece_len
    )
    weights = position_weights(local_lines, per_row, lane_count)
    master_sums = jnp.sum(master_lines * weights, axis=(1, 2)) * inv_count
    update_sums = jnp.sum(update_lines * weights, axis=(1, 2)) * inv_count

    permuting = (assignment[:, None] == span_ids[None, :]).astype(jnp.float32)
    both_sums = jnp.stack([master_sums, update_sums])
    placed_sums = jnp.sum(both_sums[:, :, None] * permuting[None], axis=1)
    entries = 2 * span_count
    tile_size = 8 * lane_count
    sums = jnp.pad(placed_sums.reshape(entries), (0, -entries % tile_size)).reshape(-1, lane_count)

    def branch_of(number, cap):
        def run(master_in, update_in):
            chosen = lists[:, :cap]
            return exchange(
                planes,
                inner,
                group_count,
                slots,
                cap,
                number_base + number,
                positions,
                sums,
                master_in[chosen],
                update_in[chosen],
            )

        return run

    saved_master, saved_update, totals = lax.switch(
        choice, [branch_of(number, cap) for number, cap in enumerate(caps)], master_lines, update_lines
    )
    checksums = totals.reshape(group_count, -1)[:, :entries].reshape(group_count, 2, span_count)
    shape_out = (1, round_count, MOST, dp_count * piece_len, lane_count)
    return (saved_master.reshape(shape_out), saved_update.reshape(shape_out), checksums)


LIST = 2
SELF = LIST + 6
NEAR = SELF + 3
DIAG = NEAR + 2
TABLES = DIAG + 1


def table_kernel(books, most_slots, rot_ref, tab_ref, choice_ref):
    rounds, _, dp_count = rot_ref.shape
    spans = rounds * dp_count
    me = lax.axis_index("dp")
    z, y, x = me // 4, (me // 2) % 2, me % 2
    mate = z + 1 - 2 * (z % 2)
    lane = lax.broadcasted_iota(jnp.int32, (1, LANE), 1)
    sub = lax.broadcasted_iota(jnp.int32, (8, LANE), 0)
    row = jnp.full((1, LANE), -1, jnp.int32)
    blocks = []
    for c in range(spans):
        if c % 8 == 0:
            block = jnp.zeros((8, LANE), jnp.int32)
        w = rot_ref[c // dp_count, 0, c % dp_count]
        row = jnp.where(lane == c, w, row)
        block = jnp.where(sub == c % 8, w, block)
        if c % 8 == 7:
            blocks.append(block)
    shape = (spans, LANE)
    writer = jnp.concatenate(blocks, axis=0)
    writer_across = jnp.broadcast_to(row, shape)
    span = lax.broadcasted_iota(jnp.int32, shape, 0)
    across = lax.broadcasted_iota(jnp.int32, shape, 1)
    before = across < span

    def rank(same):
        return jnp.sum(jnp.where(same & before, 1.0, 0.0), axis=1, keepdims=True)

    def spread(values):
        return jnp.broadcast_to(values.astype(jnp.int32), shape)

    def plane_of(w):
        return lax.shift_right_arithmetic(w, 2)

    def bit(w, n):
        return lax.shift_right_arithmetic(w, n) & 1

    plane, plane_across = plane_of(writer), plane_of(writer_across)
    same_plane = plane == plane_across
    in_plane_f = rank(same_plane)
    half_f = rank(lax.shift_right_arithmetic(writer, 3) == lax.shift_right_arithmetic(writer_across, 3))
    round_of, round_across = span // dp_count, across // dp_count
    turn = spread(rank((writer == writer_across) & (round_of == round_across)))
    outer = [jnp.sum(jnp.where(plane == p, 1, 0), axis=0, keepdims=True) for p in (0, 3)]
    in_plane = spread(in_plane_f)
    in_half = in_plane + jnp.where(plane == 1, outer[0], 0) + jnp.where(plane == 2, outer[1], 0)
    slot = round_of * most_slots + turn
    share = rounds * most_slots // 2

    def held_by(other):
        return jnp.sum(jnp.where((writer ^ other) == writer_across, 1.0, 0.0), axis=1, keepdims=True).astype(jnp.int32)

    count = [held_by(other) for other in range(4)]

    def along_x(near_x, near_y, diagonal):
        even = lax.shift_right_arithmetic(near_y + diagonal - near_x, 1)
        return jnp.minimum(jnp.maximum(even, jnp.maximum(diagonal - share, 0)), jnp.minimum(diagonal, share))

    order = rank(writer == writer_across).astype(jnp.int32)
    split = along_x(count[2], count[1], count[0])
    near = [
        order + along_x(count[0], count[3], count[2]),
        order + count[1] - along_x(count[3], count[0], count[1]),
    ]
    longest = [jnp.max((n - order + count[0]).astype(jnp.float32)) for n in near]
    by_x = order < split
    far = [jnp.where(by_x, order, LANE), jnp.where(by_x, LANE, order - split)]
    joint = jnp.where(by_x, order, share + order - split)

    def put(number, mask, value, absent):
        picked = jnp.sum(jnp.where(mask, value - absent, 0), axis=0, keepdims=True)
        tab_ref[pl.ds(number, 1), :] = picked + absent

    put(0, (lax.shift_right_arithmetic(writer, 3) != z // 2) & (in_half == across), span, 0)
    put(1, (plane == mate) & (in_plane == across), span, 0)
    for a in range(2):
        to_near, to_far = writer == (me ^ (1 + a)), writer == (me ^ 3)
        mask = (to_near & (spread(near[a]) == across)) | (to_far & (spread(far[a]) == across))
        for kind, value in enumerate((span, in_plane, in_half)):
            put(LIST + a * 3 + kind, mask, value, 0)
    at_slot = (writer == me) & (slot == across)
    places = (span, in_plane, in_half, spread(near[0]), spread(near[1]), spread(joint))
    for number, value in enumerate(places):
        put(SELF + number, at_slot, value, -1)
    is_outer = (plane == 0) | (plane == 3)
    most_half = jnp.max(half_f) + 1.0
    most_outer = jnp.max(jnp.where(is_outer, in_plane + 1, 0).astype(jnp.float32))
    most_inner = jnp.max(jnp.where(is_outer, 0, in_plane + 1).astype(jnp.float32))
    most_col = jnp.maximum(longest[0], longest[1])
    choice = jnp.int32(len(books))
    for number in reversed(range(len(books))):
        cap_half, cap_outer, cap_inner, cap_col = books[number]
        fits = (most_half <= cap_half) & (most_outer <= cap_outer)
        fits = fits & (most_inner <= cap_inner) & (most_col <= cap_col)
        choice = jnp.where(fits, number, choice)
    choice_ref[0] = choice


def tables_of(rotation, books):
    smem = pl.BlockSpec(memory_space=pltpu.SMEM)
    return pl.pallas_call(
        functools.partial(table_kernel, books, MOST),
        out_shape=(jax.ShapeDtypeStruct((TABLES, LANE), jnp.int32), jax.ShapeDtypeStruct((1,), jnp.int32)),
        in_specs=[smem],
        out_specs=(pl.BlockSpec(memory_space=pltpu.VMEM), smem),
    )(rotation.transpose(0, 2, 1))


def deliver_kernel(saved_ref, totals_ref, om_ref, ou_ref, oc_ref, held, in_sem, out_sem):
    slots = om_ref.shape[0]
    takes = []
    for f in range(2):
        for q in range(slots):
            n = f * slots + q
            takes.append(pltpu.make_async_copy(saved_ref.at[f, q], held.at[n], in_sem.at[n]))
            takes[n].start()
    oc_ref[...] = totals_ref[:, : oc_ref.shape[1], : oc_ref.shape[2]]
    gives = []
    for f, out_ref in enumerate((om_ref, ou_ref)):
        for q in range(slots):
            n = f * slots + q
            takes[n].wait()
            gives.append(pltpu.make_async_copy(held.at[n], out_ref.at[q], out_sem.at[n]))
            gives[n].start()
    for give in gives:
        give.wait()


def deliver(saved, totals, spans):
    slots = saved.shape[1]
    any_space = pl.BlockSpec(memory_space=pl.ANY)
    vmem = pl.BlockSpec(memory_space=pltpu.VMEM)
    out = jax.ShapeDtypeStruct(saved.shape[1:], jnp.float32)
    return pl.pallas_call(
        deliver_kernel,
        out_shape=(out, out, jax.ShapeDtypeStruct((totals.shape[0], 2, spans), jnp.float32)),
        in_specs=[any_space, vmem],
        out_specs=(any_space, any_space, vmem),
        scratch_shapes=[
            pltpu.VMEM((2 * slots, *saved.shape[2:]), jnp.float32),
            pltpu.SemaphoreType.DMA((2 * slots,)),
            pltpu.SemaphoreType.DMA((2 * slots,)),
        ],
        cost_estimate=pl.CostEstimate(flops=0, bytes_accessed=saved.size * 8, transcendentals=0),
        compiler_params=pltpu.CompilerParams(vmem_limit_bytes=48 * 1024 * 1024),
    )(saved, totals)


def fast_kernel(
    spans, slots, parts, lines, groups, inv_count, cap_half, cap_outer, cap_inner, cap_col,
    tab, asg_ref, wt_ref, m_ref, a_ref, b_ref, out_ref, oc_ref,
    raw_m, raw_a, raw_b, fld, xs, zs, lz, lc, fs, lf, lg, ss, work, rows_ref, sums, sums_in, across,
    load_sem, xs_sem, lc_sem, zs_sem, lz_sem, fw_sem, fs_sem, lf_sem, gs_sem, lg_sem, ss_sem, cs_sem, cr_sem,
):
    steps = 2 * parts
    ring = fs.shape[1]
    share = slots // 2
    me = lax.axis_index("dp")
    core = lax.axis_index("expert")
    z, y, x = me // 4, (me // 2) % 2, me % 2
    spot = me % 4
    inner = (z == 1) | (z == 2)
    outer = (z == 0) | (z == 3)
    outer_int = ((z + 1) // 2 + 1) % 2
    mate_x = me + 1 - 2 * x
    mate_y = me + 2 - 4 * y
    z_one = z + 1 - 2 * (z % 2)
    z_two = z + 2 - 4 * (z // 2)
    z_three = 3 - z
    mate_z = z_one * 4 + spot
    cross_to = (2 - z // 2) * 4 + spot
    plane_of = (
        z,
        z_one,
        z_two + outer_int * (z_three - z_two),
        z_three + outer_int * (z_two - z_three),
    )

    def to(dp_index):
        return (dp_index, core)

    def remote(src, dst, send, recv, target):
        return pltpu.make_async_remote_copy(
            src_ref=src,
            dst_ref=dst,
            send_sem=send,
            recv_sem=recv,
            device_id=target,
            device_id_type=pl.DeviceIdType.MESH,
        )

    loads = [
        pltpu.make_async_copy(ref, raw, load_sem.at[n])
        for n, (ref, raw) in enumerate(((m_ref, raw_m), (a_ref, raw_a), (b_ref, raw_b)))
    ]
    loads[0].start()
    barrier = pltpu.get_barrier_semaphore()
    for target in (mate_x, mate_y, mate_z, z_two * 4 + spot, z_three * 4 + spot):
        pl.semaphore_signal(barrier, inc=1, device_id=to(target), device_id_type=pl.DeviceIdType.MESH)
    for g in range(1, groups):
        pl.semaphore_signal(
            barrier, inc=1, device_id=(me, (core + g) % groups), device_id_type=pl.DeviceIdType.MESH
        )
    pl.semaphore_wait(barrier, 4 + groups)

    def relay(raw, k):
        i = k % parts

        def step(c, carry):
            row = c * parts + i
            start = (row // 8) * (8 * lines) + row % 8
            fld[k, c] = raw[pl.ds(start, lines, stride=8), :]
            return carry

        lax.fori_loop(0, spans, step, 0)

    def pick(count, row, load, store):
        def step(t, carry):
            for u in range(2):
                store(2 * t + u, load(tab[row, 2 * t + u]))
            return carry

        lax.fori_loop(0, count // 2, step, 0)
        if count % 2:
            store(count - 1, load(tab[row, count - 1]))

    def load_from(j, k):
        if j == 0:
            return lambda n: fld[k, n]
        return lambda n: work[n]

    def take(count, offset, ref, *at):
        def step(t, carry):
            for u in range(2):
                work[offset + 2 * t + u] = ref[(*at, 2 * t + u)]
            return carry

        lax.fori_loop(0, count // 2, step, 0)
        if count % 2:
            work[offset + count - 1] = ref[(*at, count - 1)]

    def cross_copy(k):
        return remote(
            xs.at[k], lc.at[1 - outer_int, k], xs_sem.at[0], lc_sem.at[1 - outer_int, k], to(cross_to)
        )

    def plane_copy(k, cap):
        some = pl.ds(0, cap)
        return remote(zs.at[k, some], lz.at[k, some], zs_sem.at[0], lz_sem.at[k], to(mate_z))

    def by_place(run):
        pl.when(inner)(lambda: run(cap_outer, cap_inner))
        pl.when(outer)(lambda: run(cap_inner, cap_outer))

    def forward_copy(s, k):
        return remote(
            lc.at[s, k, pl.ds(0, cap_outer)],
            lc.at[s, k, pl.ds(0, cap_outer)],
            fw_sem.at[0],
            lc_sem.at[s, k],
            to(mate_z),
        )

    mates = (mate_x, mate_y)
    spots = (spot, mate_x % 4, mate_y % 4, 3 - spot)

    def first_copy(a, j, k):
        r = k % ring
        return remote(fs.at[a, r, j], lf.at[a, k, j], fs_sem.at[a, r, j], lf_sem.at[a, k, j], to(mates[a]))

    def onward_copy(a, j, k):
        return remote(
            lf.at[a, k, j, pl.ds(0, share)], lg.at[a, k, j], gs_sem.at[0], lg_sem.at[a, k, j], to(mates[1 - a])
        )

    def out_copy(j, where, k):
        n = j * 4 + where
        place = out_ref.at[k // parts, :, plane_of[j] * 4 + spots[where], pl.ds((k % parts) * lines, lines)]
        return pltpu.make_async_copy(ss.at[n, k % 2], place, ss_sem.at[n, k % 2])

    def place_out(j, where, k, row, load):
        copy = out_copy(j, where, k)

        @pl.when(k >= 2)
        def _():
            copy.wait()

        for q in range(slots):
            index = tab[row, q]
            found = index >= 0
            value = load(jnp.where(found, index, 0))
            ss[j * 4 + where, k % 2, q] = jnp.where(found, value, 0.0)
        copy.start()

    def both_hops(j, k):
        kind = min(j, 2)
        for a in range(2):
            copy = first_copy(a, j, k)

            @pl.when(k >= ring)
            def _(copy=copy):
                copy.wait_send()

            def store(t, value, a=a):
                fs[a, k % ring, j, t] = value

            pick(cap_col, LIST + a * 3 + kind, load_from(j, k), store)
            copy.start()
        place_out(j, 0, k, SELF + kind, load_from(j, k))

    def near_list(j, k):
        for a in range(2):
            first_copy(a, j, k).wait_recv()
            onward_copy(a, j, k).start()
            take(cap_col, 0, lf, a, k, j)
            place_out(j, 1 + a, k, NEAR + a, load_from(1, k))

    def diag_list(j, k):
        for a in range(2):
            onward_copy(a, j, k).wait_recv()
            take(share, a * share, lg, a, k, j)
        place_out(j, 3, k, DIAG, load_from(1, k))

    def late(run, j, k, lag):
        @pl.when((k >= lag) & (k < steps + lag))
        def _():
            run(j, k - lag)

    def send_plane(k):
        def store_z(t, value):
            zs[k, t] = value

        def run(cap_out, cap_in):
            pick(cap_out, 1, load_from(0, k), store_z)
            plane_copy(k, cap_out).start()

        by_place(run)

    def own_list(raw):
        def step(k, carry):
            relay(raw, k)

            def store_x(t, value):
                xs[k, t] = value

            pick(cap_half, 0, load_from(0, k), store_x)
            cross_copy(k).start()

            send_plane(k)

            both_hops(0, k)
            return carry

        return step

    loads[0].wait()
    loads[1].start()
    loads[2].start()
    lax.fori_loop(0, parts, own_list(raw_m), 0)
    loads[1].wait()
    loads[2].wait()
    corr_one = 1.0 - BETA_ONE**STEP
    corr_two = 1.0 - BETA_TWO**STEP

    def moments(t, carry):
        at = pl.ds(t * 64, 64)
        raw_a[at, :] = raw_a[at, :] * (1.0 / corr_one) / (jnp.sqrt(raw_b[at, :] * (1.0 / corr_two)) + EPSILON)
        return carry

    lax.fori_loop(0, raw_a.shape[0] // 64, moments, 0)
    lax.fori_loop(parts, steps, own_list(raw_a), 0)

    sums[0] = jnp.zeros(sums.shape[1:], jnp.float32)
    for f in range(2):
        def one_piece(c, carry, f=f):
            total = jnp.zeros(fld.shape[2:], jnp.float32)
            for i in range(parts):
                row = (me * spans + c) * parts + i
                total = total + fld[f * parts + i, c] * wt_ref[(row * 5) % 11]
            rows_ref[pl.ds(c, 1), :] = jnp.sum(total, axis=0, keepdims=True)
            return carry

        lax.fori_loop(0, spans, one_piece, 0)
        per_span = jnp.sum(rows_ref[...], axis=1, keepdims=True) * inv_count
        rows_ref[...] = jnp.broadcast_to(per_span, rows_ref.shape)
        slot_of = lax.broadcasted_iota(jnp.int32, (1, rows_ref.shape[1]), 1)

        def one_place(c, placed):
            return placed + jnp.where(slot_of == asg_ref[c], rows_ref[pl.ds(c, 1), :], 0.0)

        sums[0, pl.ds(f, 1), :] = lax.fori_loop(0, spans, one_place, jnp.zeros(slot_of.shape, jnp.float32))

    turns = (mate_x, mate_y, mate_z, z_two * 4 + spot)

    def turn_copy(t):
        return remote(sums.at[t], sums_in.at[t], cs_sem.at[t], cr_sem.at[t], to(turns[t]))

    def turn_end(t):
        turn_copy(t).wait()
        sums[t + 1] = sums[t] + sums_in[t]

    turn_copy(0).start()

    def sums_at(k, base):
        for t in range(3):
            @pl.when(k == base + 3 * t)
            def _(t=t):
                turn_end(t)
                turn_copy(t + 1).start()

    def plane_list(j, k):
        def run(cap_out, cap_in):
            plane_copy(k, cap_in).wait_recv()
            take(cap_in, 0, lz, k)

        by_place(run)
        both_hops(1, k)

    def half_list(j, k):
        s = j - 2

        @pl.when(inner)
        def _():
            remote(xs.at[k], lc.at[s, k], xs_sem.at[0], lc_sem.at[s, k], to(cross_to)).wait_recv()
            forward_copy(s, k).start()
            take(cap_half, 0, lc, s, k)

        @pl.when(outer)
        def _():
            forward_copy(s, k).wait_recv()
            take(cap_outer, 0, lc, s, k)

        both_hops(j, k)

    slow = steps * 2 // 3

    def early_lists(k):
        late(plane_list, 1, k, 0)
        late(near_list, 0, k, 0)
        late(near_list, 1, k, 1)
        late(diag_list, 0, k, 1)
        late(diag_list, 1, k, 2)

    @pl.when(outer)
    def _():
        def step(k, carry):
            early_lists(k)
            return carry

        lax.fori_loop(0, steps + 2, step, 0)

    def arrivals(k, carry):
        @pl.when(inner)
        def _():
            early_lists(k)

        late(half_list, 2, k, 0)
        late(near_list, 2, k, 1)

        @pl.when((k >= steps) | (k % 3 > 0))
        def _():
            n = jnp.where(k < steps, k - k // 3 - 1, k - steps + slow)
            late(half_list, 3, n, 0)
            late(near_list, 3, n, 1)
            late(diag_list, 3, n, 2)

        late(diag_list, 2, k, 2)
        sums_at(k, 7)
        return carry

    lax.fori_loop(0, 2 * steps - slow + 2, arrivals, 0)

    turn_end(3)
    sent_across = []
    for g in range(1, groups):
        copy = remote(sums.at[4], across.at[g], cs_sem.at[3 + g], cr_sem.at[3 + g], (me, (core + g) % groups))
        copy.start()
        sent_across.append(copy)

    def sent(ref, sem):
        remote(ref, ref, sem.at[0], sem.at[0], to(mate_x)).wait_send()

    sent(xs, xs_sem)
    by_place(lambda cap_out, cap_in: sent(zs.at[:, pl.ds(0, cap_out)], zs_sem))
    pl.when(inner)(lambda: sent(lc.at[:, :, pl.ds(0, cap_outer)], fw_sem))
    sent(lg, gs_sem)

    def finish_ring(k, carry):
        for j in range(4):
            for a in range(2):
                first_copy(a, j, k).wait_send()
        return carry

    lax.fori_loop(steps - ring, steps, finish_ring, 0)

    def finish_own(k, carry):
        for j in range(4):
            for where in range(4):
                out_copy(j, where, k).wait()
        return carry

    lax.fori_loop(steps - 2, steps, finish_own, 0)
    oc_ref[core] = sums[4]
    for g in range(1, groups):
        sent_across[g - 1].wait()
        oc_ref[(core + groups - g) % groups] = across[g]


def fast_exchange(number, book, slots, spans, parts, lines, lanes, groups, inv_count, tab, places, weights, m_in, a_in, b_in):
    cap_half, cap_outer, cap_inner, cap_col = book
    cap_plane = max(cap_outer, cap_inner)
    steps = 2 * parts
    ring = (parts + 1) // 2
    dp_count = lax.axis_size("dp")
    share = slots // 2
    any_space = pl.BlockSpec(memory_space=pl.ANY)
    vmem = pl.BlockSpec(memory_space=pltpu.VMEM)
    smem = pl.BlockSpec(memory_space=pltpu.SMEM)

    def pieces(*lead):
        return pltpu.VMEM((*lead, lines, lanes), jnp.float32)

    def sems(*lead):
        return pltpu.SemaphoreType.DMA(lead)

    raw = pltpu.VMEM(m_in.shape, jnp.float32)
    return pl.pallas_call(
        functools.partial(fast_kernel, spans, slots, parts, lines, groups, inv_count, *book),
        out_shape=(
            jax.ShapeDtypeStruct((2, slots, dp_count, parts * lines, lanes), jnp.float32),
            jax.ShapeDtypeStruct((groups, 8, lanes), jnp.float32),
        ),
        in_specs=[smem, smem, vmem, any_space, any_space, any_space],
        out_specs=(any_space, vmem),
        scratch_shapes=[
            raw,
            raw,
            raw,
            pieces(steps, spans),
            pieces(steps, cap_half),
            pieces(steps, cap_plane),
            pieces(steps, cap_plane),
            pieces(2, steps, cap_half),
            pieces(2, ring, 4, cap_col),
            pieces(2, steps, 4, cap_col),
            pieces(2, steps, 4, share),
            pieces(16, 2, slots),
            pieces(cap_half),
            pltpu.VMEM((spans, lanes), jnp.float32),
            pltpu.VMEM((5, 8, lanes), jnp.float32),
            pltpu.VMEM((4, 8, lanes), jnp.float32),
            pltpu.VMEM((groups, 8, lanes), jnp.float32),
            sems(3),
            sems(1),
            sems(2, steps),
            sems(1),
            sems(steps),
            sems(1),
            sems(2, ring, 4),
            sems(2, steps, 4),
            sems(1),
            sems(2, steps, 4),
            sems(16, 2),
            sems(3 + groups),
            sems(3 + groups),
        ],
        cost_estimate=pl.CostEstimate(flops=0, bytes_accessed=4 * m_in.size * 8, transcendentals=0),
        compiler_params=pltpu.CompilerParams(
            collective_id=number, has_side_effects=True, vmem_limit_bytes=67043328
        ),
    )(tab, places, weights, m_in, a_in, b_in)


def shards(master, first_moment, second_moment, rotation, assignment):
    dp_count = lax.axis_size("dp")
    group_count = lax.axis_size("expert")
    round_count = rotation.shape[0]
    rows_here, columns = master.shape[1:]
    lines = columns // LANE
    span_count = round_count * dp_count
    slots = round_count * MOST
    parts = rows_here // span_count
    if dp_count != INNER * 4 or 8 * lines * (rows_here // 8) * LANE != rows_here * columns or span_count > LANE:
        return shards_general(0, False, master, first_moment, second_moment, rotation, assignment)

    half = span_count // 2
    wide = half * 7 // 8
    books = (
        (half * 9 // 8, half * 9 // 16, wide, slots),
        (half * 9 // 8, half * 3 // 4, wide, slots),
        (half * 19 // 16, half * 9 // 16, wide, slots + 1),
        (half * 19 // 16, half * 25 // 32, wide, slots + 1),
        (half * 5 // 4, half * 13 // 16, wide, slots + 2),
        (half * 43 // 32, wide, wide, slots + 3),
    )
    inv_count = 1.0 / math.sqrt(dp_count * parts * lines * LANE)
    tab, choice = tables_of(rotation, books)
    places = assignment
    pattern = np.arange(11)[:, None] + 3 * np.arange(columns)[None, :]
    weights = (1.0 + (pattern % 11).astype(np.float32) / np.float32(10.0)).astype(np.float32)
    weights = jnp.asarray(weights.reshape(11, lines, LANE))

    def tile_order(array):
        return array.reshape(rows_here // 8, 8, lines, LANE).transpose(0, 2, 1, 3).reshape(rows_here * lines, LANE)

    def fast(number, book):
        def run(tab_in, master_in, first_in, second_in):
            return fast_exchange(
                number, book, slots, span_count, parts, lines, LANE, group_count, inv_count,
                tab_in, places, weights, tile_order(master_in), tile_order(first_in), tile_order(second_in),
            )

        return run

    def general(tab_in, master_in, first_in, second_in):
        kept = shards_general(len(books), True, master_in, first_in, second_in, rotation, assignment)
        both = [saved.reshape(slots, dp_count, parts * lines, LANE) for saved in kept[:2]]
        return jnp.stack(both), jnp.pad(kept[2], ((0, 0), (0, 6), (0, LANE - span_count)))

    branches = [fast(number, book) for number, book in enumerate(books)] + [general]
    saved, totals = lax.switch(choice[0], branches, tab, master, first_moment, second_moment)
    saved_master, saved_update, checksums = deliver(saved, totals, span_count)
    shape_out = (1, round_count, MOST, dp_count * parts * lines, LANE)
    return saved_master.reshape(shape_out), saved_update.reshape(shape_out), checksums


def solution(mesh):
    placed = (P("expert", "dp", None), P("expert", "dp", None), P("expert", "dp", None), P(), P())
    return jax.shard_map(
        shards,
        mesh=mesh,
        in_specs=placed,
        out_specs=(P("expert", "dp", None, None, None), P("expert", "dp", None, None, None), P()),
        check_vma=False,
    )
```
